256 devices in a mesh: groups: 2 (over y), dom: 32 (over z, core), shot: 4 (over x).
Axes of the slice: x: 4, y: 2, z: 16, core: 2. Of those that a mesh axis runs over, the one named last changes fastest.
The devices are a block of a 4x16x16 slice.
Arguments:
- courant_sq: float32 [1024, 128, 128], P(('groups', 'dom')), parts along dimension 0, may hold values from 0.05 to 0.19
- adjoint_init: float32 [8, 2, 512, 128, 128], P(('groups', 'shot'), None, 'dom'), parts along dimension 0, may hold values from -6 to 6
- forward_saved: bfloat16 [8, 6, 512, 128, 128], P(('groups', 'shot'), None, 'dom'), parts along dimension 0, may hold values from -4 to 4
- residual_traces: float32 [8, 4, 1024], P(('groups', 'shot')), parts along dimension 0, may hold values from -6 to 6
- receivers: int32 [8, 1024, 3], P(('groups', 'shot')), parts along dimension 0, may hold values from 0 to 511, as said below
- sources: int32 [8, 3], P(('groups', 'shot')), parts along dimension 0, may hold values from 0 to 511, as said below
Outputs:
- gradient: float32 [1024, 128, 128], P(('groups', 'dom'), 'shot'), parts along dimension 0
- adjoint_final: float32 [8, 2, 512, 128, 128], P(('groups', 'shot'), None, 'dom'), parts along dimension 0
The draws below stay inside these ranges and needn't reach their ends.
There are 2 independent parts, one for each index of `groups`. The reference program is written for one: setup_inputs(seed, part) draws one part's arguments, and reference() takes and returns one part's arrays. A program takes and returns all parts, laid end to end along the dimension named above; each array names one. Nothing has to cross between parts.
Inputs may be any that keep to these rules, and one draw needn't show every extreme that they name: Each row holds the depth index (below 512), the first horizontal index (below 128) and the second (below 128) of a cell; receivers may share cells. `sources`: each row holds the depth index (below 512), the first horizontal index (below 128) and the second (below 128) of a cell.
All inputs are finite; a program needn't handle non-finite values.
Results may differ from the reference program's by a relative error of at most 0.0003.
Values sent between devices are 32-bit elements; how exact they have to be, the bound alone decides.
A program may use at most 64 MiB of HBM per device.

```python
import jax
import jax.numpy as jnp

NX = 128
NY = 128
REC = 1024
ITERS = 4
RADIUS = 6
NZ = 512
SHOTS = 4


def draw_courant_sq(key, part):
    shape = (NZ, NX, NY)
    values = jax.random.uniform(jax.random.fold_in(key, 31), shape, jnp.float32, 0.05, 0.19)
    return values


def draw_adjoint_init(key, part):
    shape = (SHOTS, 2, NZ, NX, NY)
    rough = jax.random.normal(jax.random.fold_in(key, 47), shape, jnp.float32)
    values = jnp.clip(rough, -6.0, 6.0)
    return values


def draw_receivers(key, part):
    limits = jnp.array([NZ, NX, NY], jnp.int32)
    return jax.random.randint(jax.random.fold_in(key, 11), (SHOTS, REC, 3), 0, limits).astype(jnp.int32)


def draw_sources(key, part):
    limits = jnp.array([NZ, NX, NY], jnp.int32)
    values = jax.random.randint(jax.random.fold_in(key, 23), (SHOTS, 3), 0, limits).astype(jnp.int32)
    if NZ >= max(NX, NY):
        values = values.at[0, 0].set(NZ - 1)
    elif NX >= NY:
        values = values.at[0, 1].set(NX - 1)
    else:
        values = values.at[0, 2].set(NY - 1)
    values = values.at[1, 1].set(0)
    return values.astype(jnp.int32)


def block_scale(own_key, extent, pieces, smallest, top_value):
    loudness = 1.0
    for position, blocks in pieces:
        draws = jax.random.uniform(jax.random.fold_in(jax.random.fold_in(own_key, 6), position), (blocks,), jnp.float32, smallest / len(pieces), top_value / len(pieces))
        loudness = loudness * jnp.repeat(jnp.exp(draws), extent[position] // blocks).reshape((-1,) + (1,) * (len(extent) - 1 - position))
    return loudness


def centred(stream_key, dims, scale, bound, shards=(), kind=jnp.bfloat16):
    values = jax.random.normal(stream_key, dims, jnp.float32) * scale
    if len(shards) > 0:
        values = block_scale(stream_key, dims, shards, -0.22, 0.18) * values
    return jnp.clip(values, min=-bound, max=bound).astype(kind)


def setup_inputs(seed: int = 0, part: int = 0) -> dict:
    streams_of = jax.random.split(jax.random.key(seed), 7)
    own_keys = jax.random.split(jax.random.fold_in(streams_of[6], part), 7)
    courant_sq = draw_courant_sq(jax.random.fold_in(jax.random.fold_in(streams_of[6], part), 71), part)
    adjoint_init = draw_adjoint_init(jax.random.fold_in(jax.random.fold_in(streams_of[6], part), 71), part)
    forward_saved = centred(own_keys[2], (SHOTS, ITERS + 2, NZ, NX, NY), 0.25, 4.0, ((0, 4), (2, 32)))
    residual_traces = centred(own_keys[3], (SHOTS, ITERS, REC), 1.0, 6.0, ((0, 4),), jnp.float32)
    receivers = draw_receivers(jax.random.fold_in(jax.random.fold_in(streams_of[6], part), 71), part)
    sources = draw_sources(jax.random.fold_in(jax.random.fold_in(streams_of[6], part), 71), part)
    return {"courant_sq": courant_sq, "adjoint_init": adjoint_init, "forward_saved": forward_saved, "residual_traces": residual_traces, "receivers": receivers, "sources": sources}


STENCIL_WEIGHTS = (-205.0 / 72.0, 8.0 / 5.0, -1.0 / 5.0, 8.0 / 315.0, -1.0 / 560.0)


def laplacian(field):
    size_z, size_x, size_y = field.shape
    padded = jnp.pad(field, 4)
    center = padded[4:4 + size_z, 4:4 + size_x, 4:4 + size_y]
    summed = 3.0 * STENCIL_WEIGHTS[0] * center
    for offset in range(1, 5):
        beside_all = padded[4 + offset:4 + offset + size_z, 4:4 + size_x, 4:4 + size_y]
        beside_all = beside_all + padded[4 - offset:4 - offset + size_z, 4:4 + size_x, 4:4 + size_y]
        beside_all = beside_all + padded[4:4 + size_z, 4 + offset:4 + offset + size_x, 4:4 + size_y]
        beside_all = beside_all + padded[4:4 + size_z, 4 - offset:4 - offset + size_x, 4:4 + size_y]
        beside_all = beside_all + padded[4:4 + size_z, 4:4 + size_x, 4 + offset:4 + offset + size_y]
        beside_all = beside_all + padded[4:4 + size_z, 4:4 + size_x, 4 - offset:4 - offset + size_y]
        summed = summed + STENCIL_WEIGHTS[offset] * beside_all
    return summed


def source_taper(source, depth_first, size_z, size_x, size_y):
    depth_gap = jnp.arange(size_z, dtype=jnp.int32) + depth_first - source[0]
    across_gap = jnp.arange(size_x, dtype=jnp.int32) - source[1]
    along_gap = jnp.arange(size_y, dtype=jnp.int32) - source[2]
    distance = (depth_gap * depth_gap)[:, None, None] + (across_gap * across_gap)[None, :, None] + (along_gap * along_gap)[None, None, :]
    return 1.0 - jnp.exp(-distance.astype(jnp.float32) / float(RADIUS * RADIUS))


def reference(courant_sq, adjoint_init, forward_saved, residual_traces, receivers, sources):
    size_z, size_x, size_y = courant_sq.shape
    gradient = jnp.zeros((size_z, size_x, size_y), jnp.float32)
    finals = []
    for shot_index in range(SHOTS):
        level_later = adjoint_init[shot_index, 0]
        level_now = adjoint_init[shot_index, 1]
        spots = receivers[shot_index]
        summed = jnp.zeros((size_z, size_x, size_y), jnp.float32)
        for section in range(ITERS - 1, -1, -1):
            level_next = 2.0 * level_now - level_later + courant_sq * laplacian(level_now)
            level_next = level_next.at[spots[:, 0], spots[:, 1], spots[:, 2]].add(residual_traces[shot_index, section])
            forward_accel = forward_saved[shot_index, section + 2].astype(jnp.float32) - 2.0 * forward_saved[shot_index, section + 1].astype(jnp.float32) + forward_saved[shot_index, section].astype(jnp.float32)
            summed = summed + level_next * forward_accel
            level_later, level_now = level_now, level_next
        gradient = gradient + source_taper(sources[shot_index], 0, size_z, size_x, size_y) * summed
        finals.append(jnp.stack([level_later, level_now]))
    return gradient, jnp.stack(finals)
```

```python
import functools

import jax
import jax.numpy as jnp
from jax import lax
from jax.experimental import pallas as pl
from jax.experimental.pallas import tpu as pltpu
from jax.sharding import PartitionSpec as P

ITERS = 4
RADIUS = 6
WIDTH = 4
PAD = 8
CHUNKS = 4
BLOCKS = 4
MESH = pl.DeviceIdType.MESH

SCALE = 5040.0
CENTRE = 3.0 * -14350.0
OFFSET = (0.0, 8064.0, -1008.0, 128.0, -9.0)


def kernel(
    planes,
    size_x,
    size_y,
    dom_size,
    courant_hbm,
    adjoint_hbm,
    forward_hbm,
    traces_ref,
    receivers_ref,
    source_ref,
    gradient_ref,
    final_hbm,
    lam0,
    lam1,
    lam2,
    lam3,
    lam4,
    later,
    courant,
    forward,
    along,
    band,
    spots,
    amounts,
    image,
    taper_z,
    taper_xy,
    far_halo,
    near_halo,
    got_first,
    sent_second,
    got_second,
    in_sem,
    out_sem,
    far_send,
    far_recv,
    near_send,
    near_recv,
    first_send,
    first_recv,
    second_send,
    second_recv,
):
    lam = (lam0, lam1, lam2, lam3, lam4)
    dom = lax.axis_index("dom")
    shot = lax.axis_index("shot")
    parity = dom % 2
    first_row = dom * planes
    far = dom + 2 * parity - 1
    near = dom + 1 - 2 * parity
    has_far = (far >= 0) & (far < dom_size)
    shot_a = shot + 1 - 2 * (shot % 2)
    shot_b = 3 - shot
    shot_c = (shot + 2) % 4
    rows = size_x // CHUNKS

    def depth(q):
        return q + parity * (planes - 1 - 2 * q)

    def load(kind, q):
        z = depth(q)
        if kind == 0:
            source, target = adjoint_hbm.at[0, 1, z], lam4.at[q, pl.ds(PAD, size_x)]
        elif kind == 1:
            source, target = adjoint_hbm.at[0, 0, z], later.at[q]
        elif kind == 2:
            source, target = courant_hbm.at[z], courant.at[q]
        else:
            source, target = forward_hbm.at[0, :, z], forward.at[:, q]
        return pltpu.make_async_copy(source, target, in_sem.at[kind, q])

    order = [0, 1, 2, 3] + list(range(planes - 1, 3, -1))
    for kind in range(4):
        for q in order:
            load(kind, q).start()

    barrier = pltpu.get_barrier_semaphore()
    for axis, target in (("dom", near), ("shot", shot_a), ("shot", shot_b)):
        pl.semaphore_signal(barrier, inc=1, device_id={axis: target}, device_id_type=MESH)

    @pl.when(has_far)
    def _():
        pl.semaphore_signal(barrier, inc=1, device_id={"dom": far}, device_id_type=MESH)

    for level in (1, 2, 3, 4):
        for q in range(planes):
            zero = jnp.zeros((PAD, size_y), jnp.float32)
            lam[level][q, pl.ds(0, PAD), :] = zero
            lam[level][q, pl.ds(PAD + size_x, PAD), :] = zero

    @pl.when(jnp.logical_not(has_far))
    def _():
        far_halo[...] = jnp.zeros(far_halo.shape, jnp.float32)

    row = lax.broadcasted_iota(jnp.int32, (2 * size_y, size_y), 0) % size_y
    gap = jnp.abs(row - lax.broadcasted_iota(jnp.int32, (2 * size_y, size_y), 1))
    weights = jnp.zeros(gap.shape, jnp.float32)
    for k in range(1, WIDTH + 1):
        weights = jnp.where(gap == k, OFFSET[k], weights)
    band[...] = weights.astype(jnp.bfloat16)

    @pl.when(has_far)
    def _():
        pl.semaphore_wait(barrier, 4)

    @pl.when(jnp.logical_not(has_far))
    def _():
        pl.semaphore_wait(barrier, 3)

    def far_copy(level, c):
        return pltpu.make_async_remote_copy(
            src_ref=lam[level].at[pl.ds(0, WIDTH), pl.ds(PAD + c * rows, rows)],
            dst_ref=far_halo.at[level - 1, :, pl.ds(c * rows, rows)],
            send_sem=far_send.at[level - 1, c],
            recv_sem=far_recv.at[level - 1, c],
            device_id={"dom": far},
            device_id_type=MESH,
        )

    def near_copy(level):
        return pltpu.make_async_remote_copy(
            src_ref=lam[level].at[pl.ds(planes - WIDTH, WIDTH), pl.ds(PAD, size_x)],
            dst_ref=near_halo.at[level - 1],
            send_sem=near_send.at[level - 1],
            recv_sem=near_recv.at[level - 1],
            device_id={"dom": near},
            device_id_type=MESH,
        )

    def far_start(level, c):
        @pl.when(has_far)
        def _():
            far_copy(level, c).start()

    def far_wait(level, c):
        @pl.when(has_far)
        def _():
            far_copy(level, c).wait_recv()

    for q in range(WIDTH):
        load(0, q).wait()
    for c in range(CHUNKS):
        far_start(4, c)
    for q in range(planes - WIDTH, planes):
        load(0, q).wait()
    near_copy(4).start()
    for q in range(WIDTH, planes - WIDTH):
        load(0, q).wait()

    z_index = receivers_ref[pl.ds(0, 1), :] - first_row
    z_index = z_index + parity * (planes - 1 - 2 * z_index)
    cell_row = z_index * size_x + receivers_ref[pl.ds(1, 1), :]
    count = cell_row.shape[1]

    def spots_of(block):
        base = block * WIDTH * size_x

        def body(i, carry):
            here = base + i * 16
            ids = lax.broadcasted_iota(jnp.int32, (16, count), 0) + here
            hit = jnp.where(ids == cell_row, 1.0, 0.0)
            spots[pl.ds(pl.multiple_of(here, 16), 16), :] = hit.astype(jnp.bfloat16)
            return carry

        lax.fori_loop(0, WIDTH * size_x // 16, body, 0)

    def amounts_of(step):
        value = traces_ref[pl.ds(step, 1), :]
        high = value.astype(jnp.bfloat16).astype(jnp.float32)
        low = value - high
        last = receivers_ref[pl.ds(2, 1), :]

        def body(i, carry):
            ids = lax.broadcasted_iota(jnp.int32, (16, count), 0) + i * 16
            hit = ids == last
            start = pl.multiple_of(i * 16, 16)
            amounts[step, pl.ds(start, 16), :] = jnp.where(hit, high, 0.0).astype(jnp.bfloat16)
            amounts[step, pl.ds(size_y + start, 16), :] = jnp.where(hit, low, 0.0).astype(jnp.bfloat16)
            return carry

        lax.fori_loop(0, size_y // 16, body, 0)

    def inject(step, block):
        cells = WIDTH * size_x
        both = lax.dot_general(
            spots[pl.ds(block * cells, cells), :],
            amounts[step],
            (((1,), (1,)), ((), ())),
            preferred_element_type=jnp.float32,
        )
        added = both[:, :size_y] + both[:, size_y:]
        lam[step][pl.ds(block * WIDTH, WIDTH), pl.ds(PAD, size_x), :] = added.reshape(WIDTH, size_x, size_y)

    def lateral(level, block, start, length):
        planes_here = pl.ds(block * WIDTH, WIDTH)
        field = lam[level][planes_here, pl.ds(PAD + start, length), :].reshape(WIDTH * length, size_y)
        high = field.astype(jnp.bfloat16)
        low = (field - high.astype(jnp.float32)).astype(jnp.bfloat16)
        result = jnp.dot(
            jnp.concatenate([high, low], axis=1), band[...], preferred_element_type=jnp.float32
        )
        along[planes_here, pl.ds(start, length), :] = result.reshape(WIDTH, length, size_y)

    def advance(step, block, start=0, length=size_x):
        now = lam[step + 1]
        before = later if step == 3 else lam[step + 2]
        offset = 0 if step == 3 else PAD
        low, high = block * WIDTH, (block + 1) * WIDTH
        lateral(step + 1, block, start, length)

        def body(i, carry):
            at = start + i * 8
            here = pl.ds(pl.multiple_of(at, 8), 8)
            padded = pl.ds(pl.multiple_of(at + PAD, 8), 8)
            column = {}
            for q in range(low - WIDTH, high + WIDTH):
                if 0 <= q < planes:
                    column[q] = now[q, padded, :]
                elif q >= planes:
                    column[q] = near_halo[step, WIDTH - 1 - (q - planes), here, :]
            for q in range(low, high):
                centre = column[q]
                total = along[q, here, :] + CENTRE * centre
                for k in range(1, WIDTH + 1):
                    beside = now[q, pl.ds(at + PAD + k, 8), :] + now[q, pl.ds(at + PAD - k, 8), :]
                    beside = beside + column[q + k]
                    if q - k >= 0:
                        beside = beside + column[q - k]
                    total = total + OFFSET[k] * beside
                moved = 2.0 * centre - before[q, pl.ds(pl.multiple_of(at + offset, 8), 8), :]
                scaled = courant[q, here, :] * (1.0 / SCALE)
                lam[step][q, padded, :] = lam[step][q, padded, :] + (moved + scaled * total)
            return carry

        lax.fori_loop(0, length // 8, body, 0)

    def finish(step, c):
        def body(i, carry):
            at = c * rows + i * 8
            here = pl.ds(pl.multiple_of(at, 8), 8)
            padded = pl.ds(pl.multiple_of(at + PAD, 8), 8)
            beyond = [far_halo[step, d, here, :] for d in range(WIDTH)]
            for q in range(WIDTH):
                total = OFFSET[q + 1] * beyond[0]
                for d in range(1, WIDTH - q):
                    total = total + OFFSET[q + 1 + d] * beyond[d]
                scaled = courant[q, here, :] * (1.0 / SCALE)
                lam[step][q, padded, :] = lam[step][q, padded, :] + scaled * total
            return carry

        lax.fori_loop(0, rows // 8, body, 0)

    def imaging(block):
        def body(i, carry):
            at = pl.multiple_of(i * 16, 16)
            here = pl.ds(at, 16)
            padded = pl.ds(pl.multiple_of(at + PAD, 8), 16)
            across = taper_xy[here, :]
            for q in range(block * WIDTH, (block + 1) * WIDTH):
                saved = [forward[j, q, here, :].astype(jnp.float32) for j in range(ITERS + 2)]
                total = None
                for step in range(ITERS):
                    accel = saved[step + 2] - 2.0 * saved[step + 1] + saved[step]
                    term = lam[step][q, padded, :] * accel
                    total = term if total is None else total + term
                image[q, here, :] = total * (1.0 - taper_z[pl.ds(q, 1), :] * across)
            return carry

        lax.fori_loop(0, size_x // 16, body, 0)

    piece = size_x // 4

    def first_copy(block, side, which):
        q = block * WIDTH + 2 * side
        target = (shot_a, shot_b)[side]
        part = (target, shot_c)[which]
        return pltpu.make_async_remote_copy(
            src_ref=image.at[pl.ds(q, 2), pl.ds(pl.multiple_of(part * piece, 8), piece)],
            dst_ref=got_first.at[block, side, which],
            send_sem=first_send.at[block, side, which],
            recv_sem=first_recv.at[block, side, which],
            device_id={"shot": target},
            device_id_type=MESH,
        )

    def second_copy(block, side):
        return pltpu.make_async_remote_copy(
            src_ref=sent_second.at[block, side],
            dst_ref=got_second.at[block, side],
            send_sem=second_send.at[block, side],
            recv_sem=second_recv.at[block, side],
            device_id={"shot": (shot_b, shot_a)[side]},
            device_id_type=MESH,
        )

    def reduce_start(block):
        for side in range(2):
            for which in (1, 0):
                first_copy(block, side, which).start()

    def reduce_next(block):
        for side in range(2):
            onward = (shot_b, shot_a)[side]
            q = block * WIDTH + 2 * side
            first_copy(block, side, 1).wait_recv()
            sent_second[block, side] = (
                image[pl.ds(q, 2), pl.ds(pl.multiple_of(onward * piece, 8), piece), :]
                + got_first[block, side, 1]
            )
            second_copy(block, side).start()

    def reduce_end(block):
        for side in range(2):
            first_copy(block, side, 0).wait_recv()
            second_copy(block, side).wait_recv()
            q = block * WIDTH + 2 * side
            own = image[pl.ds(q, 2), pl.ds(pl.multiple_of(shot * piece, 8), piece), :]
            own = own + got_first[block, side, 0] + got_second[block, side]
            for j in range(2):
                gradient_ref[depth(q + j)] = own[j]

    def store(level, q):
        return pltpu.make_async_copy(
            lam[level].at[q, pl.ds(PAD, size_x)], final_hbm.at[0, 1 - level, depth(q)], out_sem.at[level, q]
        )

    def store_block(level, block):
        for q in range(block * WIDTH, (block + 1) * WIDTH):
            store(level, q).start()

    def tapers():
        q_index = lax.broadcasted_iota(jnp.int32, (planes, size_y), 0)
        z_gap = q_index + parity * (planes - 1 - 2 * q_index) + first_row - source_ref[0, 0]
        taper_z[...] = jnp.exp((z_gap * z_gap).astype(jnp.float32) * (-1.0 / (RADIUS * RADIUS)))
        x_gap = lax.broadcasted_iota(jnp.int32, (size_x, size_y), 0) - source_ref[0, 1]
        y_gap = lax.broadcasted_iota(jnp.int32, (size_x, size_y), 1) - source_ref[0, 2]
        square = x_gap * x_gap + y_gap * y_gap
        taper_xy[...] = jnp.exp(square.astype(jnp.float32) * (-1.0 / (RADIUS * RADIUS)))

    amounts_of(3)
    spots_of(0)
    inject(3, 0)
    for kind in (1, 2):
        for q in order:
            load(kind, q).wait()
    advance(3, 0)
    spots_of(3)
    inject(3, 3)
    near_copy(4).wait_recv()
    advance(3, 3)
    near_copy(3).start()
    spots_of(2)
    inject(3, 2)
    advance(3, 2)
    spots_of(1)
    inject(3, 1)
    advance(3, 1)

    def wave(step, fills):
        for c in range(CHUNKS):
            far_wait(step + 1, c)
            finish(step, c)
            if step > 0:
                far_start(step, c)
                if c > 0:
                    advance(step - 1, 0, (c - 1) * rows, rows)
            if c == CHUNKS - 1 and step > 0:
                advance(step - 1, 0, c * rows, rows)
            for fill in fills[c]:
                fill()

    def full(step, block):
        inject(step, block)
        advance(step, block)

    def edge(step):
        near_copy(step + 1).wait_recv()
        full(step, 3)
        if step > 0:
            near_copy(step).start()

    def wait_forward():
        for q in order:
            load(3, q).wait()

    amounts_of(2)
    inject(2, 0)
    wave(
        3,
        [
            [lambda: edge(2)],
            [lambda: full(2, 2), lambda: amounts_of(1)],
            [lambda: edge(1), tapers],
            [lambda: inject(1, 0), lambda: full(2, 1)],
        ],
    )
    wave(
        2,
        [
            [lambda: full(1, 2), lambda: amounts_of(0)],
            [lambda: edge(0), wait_forward],
            [lambda: imaging(3), lambda: reduce_start(3)],
            [lambda: inject(0, 0), lambda: full(1, 1), lambda: reduce_next(3)],
        ],
    )
    wave(
        1,
        [
            [lambda: full(0, 2)],
            [lambda: imaging(2), lambda: reduce_start(2)],
            [lambda: reduce_end(3)],
            [lambda: full(0, 1), lambda: imaging(1), lambda: reduce_start(1), lambda: reduce_next(2)],
        ],
    )
    for block in range(BLOCKS):
        store_block(1, block)
    for block in range(1, BLOCKS):
        store_block(0, block)
    wave(0, [[lambda: reduce_next(1)], [lambda: reduce_end(2)], [], []])
    store_block(0, 0)
    imaging(0)
    reduce_start(0)
    reduce_end(1)
    reduce_next(0)
    reduce_end(0)

    for level in (1, 2, 3, 4):
        near_copy(level).wait_send()

        @pl.when(has_far)
        def _():
            for c in range(CHUNKS):
                far_copy(level, c).wait_send()

    for block in range(BLOCKS):
        for side in range(2):
            first_copy(block, side, 0).wait_send()
            first_copy(block, side, 1).wait_send()
            second_copy(block, side).wait_send()
    for level in range(2):
        for q in range(planes):
            store(level, q).wait()


def per_device(dom_size, courant_sq, adjoint_init, forward_saved, residual_traces, receivers, sources):
    planes, size_x, size_y = courant_sq.shape
    count = receivers.shape[1]
    f32, bf16 = jnp.float32, jnp.bfloat16
    padded = pltpu.VMEM((planes, size_x + 2 * PAD, size_y), f32)
    grid3 = (planes, size_x, size_y)
    dma = pltpu.SemaphoreType.DMA
    piece = (2, size_x // 4, size_y)
    return pl.pallas_call(
        functools.partial(kernel, planes, size_x, size_y, dom_size),
        out_shape=(
            jax.ShapeDtypeStruct((planes, size_x // 4, size_y), f32),
            jax.ShapeDtypeStruct((1, 2, planes, size_x, size_y), f32),
        ),
        in_specs=[pl.BlockSpec(memory_space=pl.ANY)] * 3
        + [pl.BlockSpec(memory_space=pltpu.VMEM)] * 2
        + [pl.BlockSpec(memory_space=pltpu.SMEM)],
        out_specs=(pl.BlockSpec(memory_space=pltpu.VMEM), pl.BlockSpec(memory_space=pl.ANY)),
        scratch_shapes=[padded] * 5
        + [
            pltpu.VMEM(grid3, f32),
            pltpu.VMEM(grid3, f32),
            pltpu.VMEM((ITERS + 2,) + grid3, bf16),
            pltpu.VMEM(grid3, f32),
            pltpu.VMEM((2 * size_y, size_y), bf16),
            pltpu.VMEM((planes * size_x, count), bf16),
            pltpu.VMEM((ITERS, 2 * size_y, count), bf16),
            pltpu.VMEM(grid3, f32),
            pltpu.VMEM((planes, size_y), f32),
            pltpu.VMEM((size_x, size_y), f32),
            pltpu.VMEM((ITERS, WIDTH, size_x, size_y), f32),
            pltpu.VMEM((ITERS, WIDTH, size_x, size_y), f32),
            pltpu.VMEM((BLOCKS, 2, 2) + piece, f32),
            pltpu.VMEM((BLOCKS, 2) + piece, f32),
            pltpu.VMEM((BLOCKS, 2) + piece, f32),
            dma((4, planes)),
            dma((2, planes)),
            dma((ITERS, CHUNKS)),
            dma((ITERS, CHUNKS)),
            dma((ITERS,)),
            dma((ITERS,)),
            dma((BLOCKS, 2, 2)),
            dma((BLOCKS, 2, 2)),
            dma((BLOCKS, 2)),
            dma((BLOCKS, 2)),
        ],
        compiler_params=pltpu.CompilerParams(
            collective_id=0, has_side_effects=True, vmem_limit_bytes=60 * 1024 * 1024
        ),
    )(courant_sq, adjoint_init, forward_saved, residual_traces[0], receivers[0].T, sources)


def solution(mesh):
    placed = (
        P(("groups", "dom"), None, None),
        P(("groups", "shot"), None, "dom", None, None),
        P(("groups", "shot"), None, "dom", None, None),
        P(("groups", "shot"), None, None),
        P(("groups", "shot"), None, None),
        P(("groups", "shot"), None),
    )
    return jax.shard_map(
        functools.partial(per_device, mesh.shape["dom"]),
        mesh=mesh,
        in_specs=placed,
        out_specs=(
            P(("groups", "dom"), "shot", None),
            P(("groups", "shot"), None, "dom", None, None),
        ),
        check_vma=False,
    )
```

```python
import functools

import jax
import jax.numpy as jnp
from jax import lax
from jax.experimental import pallas as pl
from jax.experimental.pallas import tpu as pltpu
from jax.sharding import PartitionSpec as P

ITERS = 4
RADIUS = 6
WIDTH = 4
PAD = 8
CHUNKS = 2
BLOCKS = 4
MESH = pl.DeviceIdType.MESH


def in_hbm(array):
    return pltpu.with_memory_space_constraint(array, pltpu.HBM)

SCALE = 5040.0
CENTRE = 3.0 * -14350.0
OFFSET = (0.0, 8064.0, -1008.0, 128.0, -9.0)


def kernel(
    planes,
    size_x,
    size_y,
    dom_size,
    courant_hbm,
    adjoint_hbm,
    forward_hbm,
    traces_hbm,
    receivers_hbm,
    source_hbm,
    gradient_ref,
    final_ref,
    traces_ref,
    receivers_ref,
    source_ref,
    lam0,
    lam1,
    lam2,
    lam3,
    lam4,
    later,
    courant,
    forward,
    along,
    band,
    spots,
    amounts,
    image,
    taper_z,
    taper_xy,
    far_halo,
    near_halo,
    got_first,
    sent_second,
    got_second,
    in_sem,
    table_sem,
    far_send,
    far_recv,
    near_send,
    near_recv,
    first_send,
    first_recv,
    second_send,
    second_recv,
):
    lam = (lam0, lam1, lam2, lam3, lam4)
    dom = lax.axis_index("dom")
    shot = lax.axis_index("shot")
    parity = dom % 2
    first_row = dom * planes
    far = dom + 2 * parity - 1
    near = dom + 1 - 2 * parity
    has_far = (far >= 0) & (far < dom_size)
    shot_a = shot + 1 - 2 * (shot % 2)
    shot_b = 3 - shot
    shot_c = (shot + 2) % 4
    rows = size_x // CHUNKS
    zero_row = (dom // dom_size) * 8

    def depth(q):
        return q + parity * (planes - 1 - 2 * q)

    def load(kind, q):
        z = depth(q)
        if kind == 0:
            source, target = adjoint_hbm.at[0, 1, z], lam4.at[q, pl.ds(PAD, size_x)]
        elif kind == 1:
            source, target = adjoint_hbm.at[0, 0, z], later.at[q]
        elif kind == 2:
            source, target = courant_hbm.at[z], courant.at[q]
        else:
            source, target = forward_hbm.at[0, :, z], forward.at[:, q]
        return pltpu.make_async_copy(source, target, in_sem.at[kind, q])

    tables = [
        pltpu.make_async_copy(source, target, table_sem.at[i])
        for i, (source, target) in enumerate(
            ((receivers_hbm, receivers_ref), (traces_hbm, traces_ref), (source_hbm, source_ref))
        )
    ]
    for table in tables:
        table.start()
    order = [0, 1, 2, 3] + list(range(planes - 1, 3, -1))
    for kind in range(4):
        for q in order:
            load(kind, q).start()

    barrier = pltpu.get_barrier_semaphore()
    for axis, target in (("dom", near), ("shot", shot_a), ("shot", shot_b)):
        pl.semaphore_signal(barrier, inc=1, device_id={axis: target}, device_id_type=MESH)

    @pl.when(has_far)
    def _():
        pl.semaphore_signal(barrier, inc=1, device_id={"dom": far}, device_id_type=MESH)

    for level in (1, 2, 3, 4):
        for q in range(planes):
            zero = jnp.zeros((PAD, size_y), jnp.float32)
            lam[level][q, pl.ds(0, PAD), :] = zero
            lam[level][q, pl.ds(PAD + size_x, PAD), :] = zero

    @pl.when(jnp.logical_not(has_far))
    def _():
        far_halo[...] = jnp.zeros(far_halo.shape, jnp.float32)

    row = lax.broadcasted_iota(jnp.int32, (2 * size_y, size_y), 0) % size_y
    gap = jnp.abs(row - lax.broadcasted_iota(jnp.int32, (2 * size_y, size_y), 1))
    weights = jnp.zeros(gap.shape, jnp.float32)
    for k in range(1, WIDTH + 1):
        weights = jnp.where(gap == k, OFFSET[k], weights)
    band[...] = weights.astype(jnp.bfloat16)

    for table in tables:
        table.wait()

    z_index = receivers_ref[0] - first_row
    z_index = z_index + parity * (planes - 1 - 2 * z_index)
    cell_row = z_index * size_x + receivers_ref[1]
    count = cell_row.shape[1]

    def spots_of():
        def body(i, carry):
            ids = lax.broadcasted_iota(jnp.int32, (16, count), 0) + i * 16
            hit = jnp.where(ids == cell_row, 1.0, 0.0)
            spots[pl.ds(pl.multiple_of(i * 16, 16), 16), :] = hit.astype(jnp.bfloat16)
            return carry

        lax.fori_loop(0, planes * size_x // 16, body, 0)

    def amounts_of(step):
        value = traces_ref[pl.ds(step, 1), :]
        high = value.astype(jnp.bfloat16).astype(jnp.float32)
        low = value - high
        last = receivers_ref[2]

        def body(i, carry):
            ids = lax.broadcasted_iota(jnp.int32, (16, count), 0) + i * 16
            hit = ids == last
            start = pl.multiple_of(i * 16, 16)
            amounts[step, pl.ds(start, 16), :] = jnp.where(hit, high, 0.0).astype(jnp.bfloat16)
            amounts[step, pl.ds(size_y + start, 16), :] = jnp.where(hit, low, 0.0).astype(jnp.bfloat16)
            return carry

        lax.fori_loop(0, size_y // 16, body, 0)

    def tapers():
        q_index = lax.broadcasted_iota(jnp.int32, (planes, size_y), 0)
        z_gap = q_index + parity * (planes - 1 - 2 * q_index) + first_row - source_ref[0, 0]
        taper_z[...] = jnp.exp((z_gap * z_gap).astype(jnp.float32) * (-1.0 / (RADIUS * RADIUS)))
        x_gap = lax.broadcasted_iota(jnp.int32, (size_x, size_y), 0) - source_ref[0, 1]
        y_gap = lax.broadcasted_iota(jnp.int32, (size_x, size_y), 1) - source_ref[0, 2]
        square = x_gap * x_gap + y_gap * y_gap
        taper_xy[...] = jnp.exp(square.astype(jnp.float32) * (-1.0 / (RADIUS * RADIUS)))

    spots_of()
    for step in range(ITERS):
        amounts_of(step)
    tapers()

    @pl.when(has_far)
    def _():
        pl.semaphore_wait(barrier, 4)

    @pl.when(jnp.logical_not(has_far))
    def _():
        pl.semaphore_wait(barrier, 3)

    def far_copy(level, c):
        return pltpu.make_async_remote_copy(
            src_ref=lam[level].at[pl.ds(0, WIDTH), pl.ds(PAD + c * rows, rows)],
            dst_ref=far_halo.at[level - 1, :, pl.ds(c * rows, rows)],
            send_sem=far_send.at[level - 1, c],
            recv_sem=far_recv.at[level - 1, c],
            device_id={"dom": far},
            device_id_type=MESH,
        )

    def near_copy(level):
        return pltpu.make_async_remote_copy(
            src_ref=lam[level].at[pl.ds(planes - WIDTH, WIDTH), pl.ds(PAD, size_x)],
            dst_ref=near_halo.at[level - 1],
            send_sem=near_send.at[level - 1],
            recv_sem=near_recv.at[level - 1],
            device_id={"dom": near},
            device_id_type=MESH,
        )

    def far_start(level, c):
        @pl.when(has_far)
        def _():
            far_copy(level, c).start()

    def far_wait(level, c):
        @pl.when(has_far)
        def _():
            far_copy(level, c).wait_recv()

    for q in range(WIDTH):
        load(0, q).wait()
    for c in range(CHUNKS):
        far_start(4, c)
    for q in range(planes - WIDTH, planes):
        load(0, q).wait()
    near_copy(4).start()

    def inject(step):
        both = lax.dot_general(
            spots[...], amounts[step], (((1,), (1,)), ((), ())), preferred_element_type=jnp.float32
        )
        added = both[:, :size_y] + both[:, size_y:]
        lam[step][:, pl.ds(PAD, size_x), :] = added.reshape(planes, size_x, size_y)

    def lateral(level, first, last):
        here = pl.ds(first * WIDTH, (last - first) * WIDTH)
        shape = ((last - first) * WIDTH, size_x, size_y)
        field = lam[level][here, pl.ds(PAD, size_x), :].reshape(-1, size_y)
        high = field.astype(jnp.bfloat16)
        low = (field - high.astype(jnp.float32)).astype(jnp.bfloat16)
        result = jnp.dot(
            jnp.concatenate([high, low], axis=1), band[...], preferred_element_type=jnp.float32
        )
        along[here, :, :] = result.reshape(shape)

    def advance(step, block):
        now = lam[step + 1]
        before = later if step == 3 else lam[step + 2]
        offset = 0 if step == 3 else PAD
        low, high = block * WIDTH, (block + 1) * WIDTH
        for i in range(size_x // 8):
            at = zero_row + i * 8
            here = pl.ds(pl.multiple_of(at, 8), 8)
            padded = pl.ds(pl.multiple_of(at + PAD, 8), 8)
            column = {}
            for q in range(low - WIDTH, high + WIDTH):
                if 0 <= q < planes:
                    column[q] = now[q, padded, :]
                elif q >= planes:
                    column[q] = near_halo[step, WIDTH - 1 - (q - planes), here, :]
            for q in range(low, high):
                centre = column[q]
                total = along[q, here, :] + CENTRE * centre
                for k in range(1, WIDTH + 1):
                    beside = now[q, pl.ds(at + PAD + k, 8), :] + now[q, pl.ds(at + PAD - k, 8), :]
                    beside = beside + column[q + k]
                    if q - k >= 0:
                        beside = beside + column[q - k]
                    total = total + OFFSET[k] * beside
                moved = 2.0 * centre - before[q, pl.ds(pl.multiple_of(at + offset, 8), 8), :]
                scaled = courant[q, here, :] * (1.0 / SCALE)
                lam[step][q, padded, :] = lam[step][q, padded, :] + (moved + scaled * total)

    def finish(step, c):
        for i in range(rows // 8):
            at = zero_row + c * rows + i * 8
            here = pl.ds(pl.multiple_of(at, 8), 8)
            padded = pl.ds(pl.multiple_of(at + PAD, 8), 8)
            beyond = [far_halo[step, d, here, :] for d in range(WIDTH)]
            for q in range(WIDTH):
                total = OFFSET[q + 1] * beyond[0]
                for d in range(1, WIDTH - q):
                    total = total + OFFSET[q + 1 + d] * beyond[d]
                scaled = courant[q, here, :] * (1.0 / SCALE)
                lam[step][q, padded, :] = lam[step][q, padded, :] + scaled * total

    def imaging(block):
        def body(i, carry):
            at = pl.multiple_of(i * 16, 16)
            here = pl.ds(at, 16)
            padded = pl.ds(pl.multiple_of(at + PAD, 8), 16)
            across = taper_xy[here, :]
            for q in range(block * WIDTH, (block + 1) * WIDTH):
                saved = [forward[j, q, here, :].astype(jnp.float32) for j in range(ITERS + 2)]
                total = None
                for step in range(ITERS):
                    accel = saved[step + 2] - 2.0 * saved[step + 1] + saved[step]
                    term = lam[step][q, padded, :] * accel
                    total = term if total is None else total + term
                image[q, here, :] = total * (1.0 - taper_z[pl.ds(q, 1), :] * across)
            return carry

        lax.fori_loop(0, size_x // 16, body, 0)

    piece = size_x // 4

    def first_copy(block, side, which):
        q = block * WIDTH + 2 * side
        target = (shot_a, shot_b)[side]
        part = (target, shot_c)[which]
        return pltpu.make_async_remote_copy(
            src_ref=image.at[pl.ds(q, 2), pl.ds(pl.multiple_of(part * piece, 8), piece)],
            dst_ref=got_first.at[block, side, which],
            send_sem=first_send.at[block, side, which],
            recv_sem=first_recv.at[block, side, which],
            device_id={"shot": target},
            device_id_type=MESH,
        )

    def second_copy(block, side):
        return pltpu.make_async_remote_copy(
            src_ref=sent_second.at[block, side],
            dst_ref=got_second.at[block, side],
            send_sem=second_send.at[block, side],
            recv_sem=second_recv.at[block, side],
            device_id={"shot": (shot_b, shot_a)[side]},
            device_id_type=MESH,
        )

    def reduce_start(block):
        for side in range(2):
            for which in (1, 0):
                first_copy(block, side, which).start()

    def reduce_next(block):
        for side in range(2):
            onward = (shot_b, shot_a)[side]
            q = block * WIDTH + 2 * side
            first_copy(block, side, 1).wait_recv()
            sent_second[block, side] = (
                image[pl.ds(q, 2), pl.ds(pl.multiple_of(onward * piece, 8), piece), :]
                + got_first[block, side, 1]
            )
            second_copy(block, side).start()

    def reduce_end(block):
        for side in range(2):
            first_copy(block, side, 0).wait_recv()
            second_copy(block, side).wait_recv()
            q = block * WIDTH + 2 * side
            own = image[pl.ds(q, 2), pl.ds(pl.multiple_of(shot * piece, 8), piece), :]
            own = own + got_first[block, side, 0] + got_second[block, side]
            for j in range(2):
                gradient_ref[depth(q + j)] = own[j]

    def store(level, block):
        for q in range(block * WIDTH, (block + 1) * WIDTH):
            final_ref[1 - level, depth(q)] = lam[level][q, pl.ds(PAD, size_x), :]

    def wait_near(level):
        near_copy(level).wait_recv()

    def wave(step, first, second):
        for c, fill in enumerate((first, second)):
            far_wait(step + 1, c)
            finish(step, c)
            if step > 0:
                far_start(step, c)
            fill()

    inject(3)
    for q in range(WIDTH, planes - WIDTH):
        load(0, q).wait()
    for kind in (1, 2):
        for q in order:
            load(kind, q).wait()
    lateral(4, 0, 4)
    advance(3, 0)
    advance(3, 2)
    wait_near(4)
    advance(3, 3)
    near_copy(3).start()
    advance(3, 1)

    def first_3():
        lateral(3, 1, 4)
        inject(2)
        advance(2, 2)
        wait_near(3)
        advance(2, 3)
        near_copy(2).start()

    def second_3():
        lateral(3, 0, 1)
        inject(1)
        advance(2, 0)
        lateral(2, 3, 4)
        advance(2, 1)
        wait_near(2)
        advance(1, 3)
        near_copy(1).start()

    def first_2():
        lateral(2, 1, 3)
        inject(0)
        advance(1, 2)
        for q in order:
            load(3, q).wait()

    def second_2():
        lateral(2, 0, 1)
        lateral(1, 3, 4)
        advance(1, 0)
        advance(1, 1)
        wait_near(1)
        advance(0, 3)
        imaging(3)
        reduce_start(3)

    def first_1():
        lateral(1, 1, 3)
        advance(0, 2)
        imaging(2)
        reduce_start(2)
        reduce_next(3)

    def second_1():
        lateral(1, 0, 1)
        advance(0, 1)
        imaging(1)
        reduce_start(1)
        advance(0, 0)
        reduce_next(2)
        for block in range(1, BLOCKS):
            store(0, block)

    wave(3, first_3, second_3)
    wave(2, first_2, second_2)
    wave(1, first_1, second_1)
    wave(0, lambda: None, lambda: None)
    imaging(0)
    reduce_start(0)
    store(0, 0)
    for block in range(BLOCKS):
        store(1, block)
    reduce_end(3)
    reduce_next(1)
    reduce_end(2)
    reduce_next(0)
    reduce_end(1)
    reduce_end(0)

    for level in (1, 2, 3, 4):
        near_copy(level).wait_send()

        @pl.when(has_far)
        def _():
            for c in range(CHUNKS):
                far_copy(level, c).wait_send()

    for block in range(BLOCKS):
        for side in range(2):
            first_copy(block, side, 0).wait_send()
            first_copy(block, side, 1).wait_send()
            second_copy(block, side).wait_send()

def write_out(gradient_ref, final_ref, gradient_hbm, final_hbm, sem):
    copies = [pltpu.make_async_copy(gradient_ref, gradient_hbm, sem.at[0])]
    half = final_ref.shape[1] // 2
    for level in range(2):
        for part in range(2):
            at = pl.ds(part * half, half)
            copies.append(
                pltpu.make_async_copy(
                    final_ref.at[level, at], final_hbm.at[0, level, at], sem.at[1 + 2 * level + part]
                )
            )
    for copy in copies:
        copy.start()
    for copy in copies:
        copy.wait()


def per_device(dom_size, courant_sq, adjoint_init, forward_saved, residual_traces, receivers, sources):
    planes, size_x, size_y = courant_sq.shape
    count = receivers.shape[1]
    f32, bf16 = jnp.float32, jnp.bfloat16
    padded = pltpu.VMEM((planes, size_x + 2 * PAD, size_y), f32)
    grid3 = (planes, size_x, size_y)
    dma = pltpu.SemaphoreType.DMA
    piece = (2, size_x // 4, size_y)
    gradient, final = pl.pallas_call(
        functools.partial(kernel, planes, size_x, size_y, dom_size),
        out_shape=(
            jax.ShapeDtypeStruct((planes, size_x // 4, size_y), f32),
            jax.ShapeDtypeStruct((2, planes, size_x, size_y), f32),
        ),
        in_specs=[pl.BlockSpec(memory_space=pltpu.HBM)] * 6,
        out_specs=(pl.BlockSpec(memory_space=pltpu.VMEM), pl.BlockSpec(memory_space=pltpu.VMEM)),
        scratch_shapes=[
            pltpu.VMEM((ITERS, count), f32),
            pltpu.VMEM((3, 1, count), jnp.int32),
            pltpu.SMEM((1, 3), jnp.int32),
        ]
        + [padded] * 5
        + [
            pltpu.VMEM(grid3, f32),
            pltpu.VMEM(grid3, f32),
            pltpu.VMEM((ITERS + 2,) + grid3, bf16),
            pltpu.VMEM(grid3, f32),
            pltpu.VMEM((2 * size_y, size_y), bf16),
            pltpu.VMEM((planes * size_x, count), bf16),
            pltpu.VMEM((ITERS, 2 * size_y, count), bf16),
            pltpu.VMEM(grid3, f32),
            pltpu.VMEM((planes, size_y), f32),
            pltpu.VMEM((size_x, size_y), f32),
            pltpu.VMEM((ITERS, WIDTH, size_x, size_y), f32),
            pltpu.VMEM((ITERS, WIDTH, size_x, size_y), f32),
            pltpu.VMEM((BLOCKS, 2, 2) + piece, f32),
            pltpu.VMEM((BLOCKS, 2) + piece, f32),
            pltpu.VMEM((BLOCKS, 2) + piece, f32),
            dma((4, planes)),
            dma((3,)),
            dma((ITERS, CHUNKS)),
            dma((ITERS, CHUNKS)),
            dma((ITERS,)),
            dma((ITERS,)),
            dma((BLOCKS, 2, 2)),
            dma((BLOCKS, 2, 2)),
            dma((BLOCKS, 2)),
            dma((BLOCKS, 2)),
        ],
        compiler_params=pltpu.CompilerParams(
            collective_id=0, has_side_effects=True, vmem_limit_bytes=34 * 1024 * 1024
        ),
    )(
        *(
            in_hbm(array)
            for array in (
                courant_sq,
                adjoint_init,
                forward_saved,
                residual_traces[0],
                receivers.transpose(2, 0, 1),
                sources,
            )
        )
    )
    return pl.pallas_call(
        write_out,
        out_shape=(
            jax.ShapeDtypeStruct(gradient.shape, f32),
            jax.ShapeDtypeStruct((1,) + final.shape, f32),
        ),
        in_specs=[pl.BlockSpec(memory_space=pltpu.VMEM)] * 2,
        out_specs=(pl.BlockSpec(memory_space=pl.ANY),) * 2,
        scratch_shapes=[dma((5,))],
        compiler_params=pltpu.CompilerParams(vmem_limit_bytes=8 * 1024 * 1024),
    )(gradient, final)


def solution(mesh):
    placed = (
        P(("groups", "dom"), None, None),
        P(("groups", "shot"), None, "dom", None, None),
        P(("groups", "shot"), None, "dom", None, None),
        P(("groups", "shot"), None, None),
        P(("groups", "shot"), None, None),
        P(("groups", "shot"), None),
    )
    return jax.shard_map(
        functools.partial(per_device, mesh.shape["dom"]),
        mesh=mesh,
        in_specs=placed,
        out_specs=(
            P(("groups", "dom"), "shot", None),
            P(("groups", "shot"), None, "dom", None, None),
        ),
        check_vma=False,
    )
```

```python
import functools

import jax
import jax.numpy as jnp
from jax import lax
from jax.experimental import pallas as pl
from jax.experimental.pallas import tpu as pltpu
from jax.sharding import PartitionSpec as P

ITERS = 4
RADIUS = 6
WIDTH = 4
PAD = 8
CHUNKS = 4
BLOCKS = 4
MESH = pl.DeviceIdType.MESH


def in_hbm(array):
    return pltpu.with_memory_space_constraint(array, pltpu.HBM)

SCALE = 5040.0
CENTRE = 3.0 * -14350.0
OFFSET = (0.0, 8064.0, -1008.0, 128.0, -9.0)


def kernel(
    planes,
    size_x,
    size_y,
    dom_size,
    courant_hbm,
    adjoint_hbm,
    forward_hbm,
    traces_hbm,
    receivers_hbm,
    source_hbm,
    gradient_ref,
    final_ref,
    traces_ref,
    receivers_ref,
    source_ref,
    lam0,
    lam1,
    lam2,
    lam3,
    lam4,
    later,
    courant,
    forward,
    along,
    band,
    spots,
    across,
    amounts,
    image,
    taper_z,
    taper_xy,
    far_halo,
    near_halo,
    got_first,
    sent_second,
    got_second,
    in_sem,
    table_sem,
    far_send,
    far_recv,
    near_send,
    near_recv,
    first_send,
    first_recv,
    second_send,
    second_recv,
):
    lam = (lam0, lam1, lam2, lam3, lam4)
    dom = lax.axis_index("dom")
    shot = lax.axis_index("shot")
    parity = dom % 2
    first_row = dom * planes
    far = dom + 2 * parity - 1
    near = dom + 1 - 2 * parity
    has_far = (far >= 0) & (far < dom_size)
    shot_a = shot + 1 - 2 * (shot % 2)
    shot_b = 3 - shot
    shot_c = (shot + 2) % 4
    rows = size_x // CHUNKS
    zero_row = (dom // dom_size) * 8

    def depth(q):
        return q + parity * (planes - 1 - 2 * q)

    def load(kind, q):
        z = depth(q)
        if kind == 0:
            source, target = adjoint_hbm.at[0, 1, z], lam4.at[q, pl.ds(PAD, size_x)]
        elif kind == 1:
            source, target = adjoint_hbm.at[0, 0, z], later.at[q]
        elif kind == 2:
            source, target = courant_hbm.at[z], courant.at[q]
        else:
            source, target = forward_hbm.at[0, :, z], forward.at[:, q]
        return pltpu.make_async_copy(source, target, in_sem.at[kind, q])

    barrier = pltpu.get_barrier_semaphore()
    for axis, target in (("dom", near), ("shot", shot_a), ("shot", shot_b)):
        pl.semaphore_signal(barrier, inc=1, device_id={axis: target}, device_id_type=MESH)

    @pl.when(has_far)
    def _():
        pl.semaphore_signal(barrier, inc=1, device_id={"dom": far}, device_id_type=MESH)

    tables = [
        pltpu.make_async_copy(source, target, table_sem.at[i])
        for i, (source, target) in enumerate(
            ((receivers_hbm, receivers_ref), (traces_hbm, traces_ref), (source_hbm, source_ref))
        )
    ]
    for table in tables:
        table.start()
    order = [0, 1, 2, 3] + list(range(planes - 1, 3, -1))
    for kind in range(4):
        for q in order:
            load(kind, q).start()

    for level in (1, 2, 3, 4):
        for q in range(planes):
            zero = jnp.zeros((PAD, size_y), jnp.float32)
            lam[level][q, pl.ds(0, PAD), :] = zero
            lam[level][q, pl.ds(PAD + size_x, PAD), :] = zero

    @pl.when(jnp.logical_not(has_far))
    def _():
        far_halo[...] = jnp.zeros(far_halo.shape, jnp.float32)

    row = lax.broadcasted_iota(jnp.int32, (2 * size_y, size_y), 0) % size_y
    gap = jnp.abs(row - lax.broadcasted_iota(jnp.int32, (2 * size_y, size_y), 1))
    weights = jnp.zeros(gap.shape, jnp.float32)
    for k in range(1, WIDTH + 1):
        weights = jnp.where(gap == k, OFFSET[k], weights)
    band[...] = weights.astype(jnp.bfloat16)

    for table in tables[:2]:
        table.wait()

    z_index = receivers_ref[0] - first_row
    z_index = z_index + parity * (planes - 1 - 2 * z_index)
    count = z_index.shape[1]

    def spots_of():
        ids = lax.broadcasted_iota(jnp.int32, (size_x, count), 0)
        across[...] = jnp.where(ids == receivers_ref[1], 1.0, 0.0).astype(jnp.bfloat16)
        for q in range(planes):
            level = jnp.where(z_index == q, 1.0, 0.0).astype(jnp.bfloat16)
            spots[pl.ds(q * size_x, size_x), :] = across[...] * level

    def amounts_of(step):
        value = traces_ref[pl.ds(step, 1), :]
        high = value.astype(jnp.bfloat16).astype(jnp.float32)
        low = value - high
        last = receivers_ref[2]

        def body(i, carry):
            ids = lax.broadcasted_iota(jnp.int32, (16, count), 0) + i * 16
            hit = ids == last
            start = pl.multiple_of(i * 16, 16)
            amounts[step, pl.ds(start, 16), :] = jnp.where(hit, high, 0.0).astype(jnp.bfloat16)
            amounts[step, pl.ds(size_y + start, 16), :] = jnp.where(hit, low, 0.0).astype(jnp.bfloat16)
            return carry

        lax.fori_loop(0, size_y // 16, body, 0)

    def tapers():
        tables[2].wait()
        q_index = lax.broadcasted_iota(jnp.int32, (planes, size_y), 0)
        z_gap = q_index + parity * (planes - 1 - 2 * q_index) + first_row - source_ref[0, 0]
        taper_z[...] = jnp.exp((z_gap * z_gap).astype(jnp.float32) * (-1.0 / (RADIUS * RADIUS)))
        x_gap = lax.broadcasted_iota(jnp.int32, (size_x, size_y), 0) - source_ref[0, 1]
        y_gap = lax.broadcasted_iota(jnp.int32, (size_x, size_y), 1) - source_ref[0, 2]
        square = x_gap * x_gap + y_gap * y_gap
        taper_xy[...] = jnp.exp(square.astype(jnp.float32) * (-1.0 / (RADIUS * RADIUS)))

    spots_of()
    amounts_of(3)

    @pl.when(has_far)
    def _():
        pl.semaphore_wait(barrier, 4)

    @pl.when(jnp.logical_not(has_far))
    def _():
        pl.semaphore_wait(barrier, 3)

    def far_copy(level, c):
        return pltpu.make_async_remote_copy(
            src_ref=lam[level].at[pl.ds(0, WIDTH), pl.ds(PAD + c * rows, rows)],
            dst_ref=far_halo.at[level - 1, :, pl.ds(c * rows, rows)],
            send_sem=far_send.at[level - 1, c],
            recv_sem=far_recv.at[level - 1, c],
            device_id={"dom": far},
            device_id_type=MESH,
        )

    def near_copy(level):
        return pltpu.make_async_remote_copy(
            src_ref=lam[level].at[pl.ds(planes - WIDTH, WIDTH), pl.ds(PAD, size_x)],
            dst_ref=near_halo.at[level - 1],
            send_sem=near_send.at[level - 1],
            recv_sem=near_recv.at[level - 1],
            device_id={"dom": near},
            device_id_type=MESH,
        )

    def far_start(level, c):
        @pl.when(has_far)
        def _():
            far_copy(level, c).start()

    def far_wait(level, c):
        @pl.when(has_far)
        def _():
            far_copy(level, c).wait_recv()

    for q in range(WIDTH):
        load(0, q).wait()
    for c in range(CHUNKS):
        far_start(4, c)
    for q in range(planes - WIDTH, planes):
        load(0, q).wait()
    near_copy(4).start()

    def inject(step, first, last):
        half = (last - first) * WIDTH // 2
        for part in range(2):
            start = first * WIDTH + part * half
            both = lax.dot_general(
                spots[pl.ds(start * size_x, half * size_x), :],
                amounts[step],
                (((1,), (1,)), ((), ())),
                preferred_element_type=jnp.float32,
            )
            added = both[:, :size_y] + both[:, size_y:]
            lam[step][pl.ds(start, half), pl.ds(PAD, size_x), :] = added.reshape(half, size_x, size_y)

    def lateral(level, first, last):
        here = pl.ds(first * WIDTH, (last - first) * WIDTH)
        shape = ((last - first) * WIDTH, size_x, size_y)
        field = lam[level][here, pl.ds(PAD, size_x), :].reshape(-1, size_y)
        high = field.astype(jnp.bfloat16)
        low = (field - high.astype(jnp.float32)).astype(jnp.bfloat16)
        result = jnp.dot(
            jnp.concatenate([high, low], axis=1), band[...], preferred_element_type=jnp.float32
        )
        along[here, :, :] = result.reshape(shape)

    def advance(step, block):
        now = lam[step + 1]
        before = later if step == 3 else lam[step + 2]
        offset = 0 if step == 3 else PAD
        low, high = block * WIDTH, (block + 1) * WIDTH
        for i in range(size_x // 8):
            at = zero_row + i * 8
            here = pl.ds(pl.multiple_of(at, 8), 8)
            padded = pl.ds(pl.multiple_of(at + PAD, 8), 8)
            column = {}
            for q in range(low - WIDTH, high + WIDTH):
                if 0 <= q < planes:
                    column[q] = now[q, padded, :]
                elif q >= planes:
                    column[q] = near_halo[step, WIDTH - 1 - (q - planes), here, :]
            for q in range(low, high):
                centre = column[q]
                total = along[q, here, :] + CENTRE * centre
                for k in range(1, WIDTH + 1):
                    beside = now[q, pl.ds(at + PAD + k, 8), :] + now[q, pl.ds(at + PAD - k, 8), :]
                    beside = beside + column[q + k]
                    if q - k >= 0:
                        beside = beside + column[q - k]
                    total = total + OFFSET[k] * beside
                moved = 2.0 * centre - before[q, pl.ds(pl.multiple_of(at + offset, 8), 8), :]
                scaled = courant[q, here, :] * (1.0 / SCALE)
                lam[step][q, padded, :] = lam[step][q, padded, :] + (moved + scaled * total)

    def finish(step, c):
        for i in range(rows // 8):
            at = zero_row + c * rows + i * 8
            here = pl.ds(pl.multiple_of(at, 8), 8)
            padded = pl.ds(pl.multiple_of(at + PAD, 8), 8)
            beyond = [far_halo[step, d, here, :] for d in range(WIDTH)]
            for q in range(WIDTH):
                total = OFFSET[q + 1] * beyond[0]
                for d in range(1, WIDTH - q):
                    total = total + OFFSET[q + 1 + d] * beyond[d]
                scaled = courant[q, here, :] * (1.0 / SCALE)
                lam[step][q, padded, :] = lam[step][q, padded, :] + scaled * total

    def imaging(block):
        def body(i, carry):
            at = pl.multiple_of(i * 16, 16)
            here = pl.ds(at, 16)
            padded = pl.ds(pl.multiple_of(at + PAD, 8), 16)
            across = taper_xy[here, :]
            for q in range(block * WIDTH, (block + 1) * WIDTH):
                saved = [forward[j, q, here, :].astype(jnp.float32) for j in range(ITERS + 2)]
                total = None
                for step in range(ITERS):
                    accel = saved[step + 2] - 2.0 * saved[step + 1] + saved[step]
                    term = lam[step][q, padded, :] * accel
                    total = term if total is None else total + term
                image[q, here, :] = total * (1.0 - taper_z[pl.ds(q, 1), :] * across)
            return carry

        lax.fori_loop(0, size_x // 16, body, 0)

    piece = size_x // 4

    def first_copy(block, side, which):
        q = block * WIDTH + 2 * side
        target = (shot_a, shot_b)[side]
        part = (target, shot_c)[which]
        return pltpu.make_async_remote_copy(
            src_ref=image.at[pl.ds(q, 2), pl.ds(pl.multiple_of(part * piece, 8), piece)],
            dst_ref=got_first.at[block, side, which],
            send_sem=first_send.at[block, side, which],
            recv_sem=first_recv.at[block, side, which],
            device_id={"shot": target},
            device_id_type=MESH,
        )

    def second_copy(block, side):
        return pltpu.make_async_remote_copy(
            src_ref=sent_second.at[block, side],
            dst_ref=got_second.at[block, side],
            send_sem=second_send.at[block, side],
            recv_sem=second_recv.at[block, side],
            device_id={"shot": (shot_b, shot_a)[side]},
            device_id_type=MESH,
        )

    def reduce_start(block, which):
        for side in range(2):
            first_copy(block, side, which).start()

    def reduce_next(block):
        for side in range(2):
            onward = (shot_b, shot_a)[side]
            q = block * WIDTH + 2 * side
            first_copy(block, side, 1).wait_recv()
            sent_second[block, side] = (
                image[pl.ds(q, 2), pl.ds(pl.multiple_of(onward * piece, 8), piece), :]
                + got_first[block, side, 1]
            )
            second_copy(block, side).start()

    def reduce_end(block):
        for side in range(2):
            first_copy(block, side, 0).wait_recv()
            second_copy(block, side).wait_recv()
            q = block * WIDTH + 2 * side
            own = image[pl.ds(q, 2), pl.ds(pl.multiple_of(shot * piece, 8), piece), :]
            own = own + got_first[block, side, 0] + got_second[block, side]
            for j in range(2):
                gradient_ref[depth(q + j)] = own[j]

    def store(level, block):
        for q in range(block * WIDTH, (block + 1) * WIDTH):
            final_ref[1 - level, depth(q)] = lam[level][q, pl.ds(PAD, size_x), :]

    def wait_near(level):
        near_copy(level).wait_recv()

    def take(step, c):
        far_wait(step + 1, c)
        finish(step, c)
        if step > 0:
            far_start(step, c)

    def edge(step):
        wait_near(step + 1)
        advance(step, 3)
        if step > 0:
            near_copy(step).start()

    inject(3, 0, 4)
    for q in range(WIDTH, planes - WIDTH):
        load(0, q).wait()
    for kind in (1, 2):
        for q in order:
            load(kind, q).wait()
    lateral(4, 0, 4)
    advance(3, 0)
    edge(3)
    take(3, 0)
    advance(3, 2)
    amounts_of(2)
    take(3, 1)
    advance(3, 1)
    amounts_of(1)
    take(3, 2)
    inject(2, 0, 4)
    take(3, 3)

    lateral(3, 0, 4)
    advance(2, 0)
    take(2, 0)
    edge(2)
    advance(2, 2)
    take(2, 1)
    advance(2, 1)
    amounts_of(0)
    take(2, 2)
    inject(1, 0, 4)
    take(2, 3)

    lateral(2, 0, 4)
    advance(1, 0)
    take(1, 0)
    edge(1)
    advance(1, 2)
    take(1, 1)
    inject(0, 2, 4)
    lateral(1, 2, 4)
    edge(0)
    tapers()
    for q in order:
        load(3, q).wait()
    imaging(3)
    reduce_start(3, 1)
    reduce_start(3, 0)
    take(1, 2)
    advance(1, 1)
    inject(0, 0, 2)
    take(1, 3)

    lateral(1, 0, 2)
    advance(0, 2)
    imaging(2)
    reduce_start(2, 1)
    reduce_start(2, 0)
    advance(0, 0)
    take(0, 0)
    advance(0, 1)
    imaging(1)
    reduce_start(1, 1)
    take(0, 1)
    for block in range(BLOCKS):
        store(1, block)
    for block in range(1, BLOCKS):
        store(0, block)
    take(0, 2)
    reduce_next(3)
    take(0, 3)
    imaging(0)
    reduce_start(0, 1)
    reduce_start(1, 0)
    reduce_start(0, 0)
    store(0, 0)
    reduce_next(2)
    reduce_next(1)
    for level in (1, 2, 3, 4):
        near_copy(level).wait_send()

        @pl.when(has_far)
        def _():
            for c in range(CHUNKS):
                far_copy(level, c).wait_send()

    reduce_next(0)
    reduce_end(3)
    reduce_end(2)
    reduce_end(1)
    for block in range(BLOCKS):
        for side in range(2):
            first_copy(block, side, 0).wait_send()
            first_copy(block, side, 1).wait_send()
            second_copy(block, side).wait_send()
    reduce_end(0)


def write_out(gradient_ref, final_ref, gradient_hbm, final_hbm, sem):
    copies = [pltpu.make_async_copy(gradient_ref, gradient_hbm, sem.at[0])]
    half = final_ref.shape[1] // 2
    for level in range(2):
        for part in range(2):
            at = pl.ds(part * half, half)
            copies.append(
                pltpu.make_async_copy(
                    final_ref.at[level, at], final_hbm.at[0, level, at], sem.at[1 + 2 * level + part]
                )
            )
    for copy in copies:
        copy.start()
    for copy in copies:
        copy.wait()


def per_device(dom_size, courant_sq, adjoint_init, forward_saved, residual_traces, receivers, sources):
    planes, size_x, size_y = courant_sq.shape
    count = receivers.shape[1]
    f32, bf16 = jnp.float32, jnp.bfloat16
    padded = pltpu.VMEM((planes, size_x + 2 * PAD, size_y), f32)
    grid3 = (planes, size_x, size_y)
    dma = pltpu.SemaphoreType.DMA
    piece = (2, size_x // 4, size_y)
    gradient, final = pl.pallas_call(
        functools.partial(kernel, planes, size_x, size_y, dom_size),
        out_shape=(
            jax.ShapeDtypeStruct((planes, size_x // 4, size_y), f32),
            jax.ShapeDtypeStruct((2, planes, size_x, size_y), f32),
        ),
        in_specs=[pl.BlockSpec(memory_space=pltpu.HBM)] * 6,
        out_specs=(pl.BlockSpec(memory_space=pltpu.VMEM), pl.BlockSpec(memory_space=pltpu.VMEM)),
        scratch_shapes=[
            pltpu.VMEM((ITERS, count), f32),
            pltpu.VMEM((3, 1, count), jnp.int32),
            pltpu.SMEM((1, 3), jnp.int32),
        ]
        + [padded] * 5
        + [
            pltpu.VMEM(grid3, f32),
            pltpu.VMEM(grid3, f32),
            pltpu.VMEM((ITERS + 2,) + grid3, bf16),
            pltpu.VMEM(grid3, f32),
            pltpu.VMEM((2 * size_y, size_y), bf16),
            pltpu.VMEM((planes * size_x, count), bf16),
            pltpu.VMEM((size_x, count), bf16),
            pltpu.VMEM((ITERS, 2 * size_y, count), bf16),
            pltpu.VMEM(grid3, f32),
            pltpu.VMEM((planes, size_y), f32),
            pltpu.VMEM((size_x, size_y), f32),
            pltpu.VMEM((ITERS, WIDTH, size_x, size_y), f32),
            pltpu.VMEM((ITERS, WIDTH, size_x, size_y), f32),
            pltpu.VMEM((BLOCKS, 2, 2) + piece, f32),
            pltpu.VMEM((BLOCKS, 2) + piece, f32),
            pltpu.VMEM((BLOCKS, 2) + piece, f32),
            dma((4, planes)),
            dma((3,)),
            dma((ITERS, CHUNKS)),
            dma((ITERS, CHUNKS)),
            dma((ITERS,)),
            dma((ITERS,)),
            dma((BLOCKS, 2, 2)),
            dma((BLOCKS, 2, 2)),
            dma((BLOCKS, 2)),
            dma((BLOCKS, 2)),
        ],
        compiler_params=pltpu.CompilerParams(
            collective_id=0, has_side_effects=True, vmem_limit_bytes=34 * 1024 * 1024
        ),
    )(
        *(
            in_hbm(array)
            for array in (
                courant_sq,
                adjoint_init,
                forward_saved,
                residual_traces[0],
                receivers.transpose(2, 0, 1),
                sources,
            )
        )
    )
    return pl.pallas_call(
        write_out,
        out_shape=(
            jax.ShapeDtypeStruct(gradient.shape, f32),
            jax.ShapeDtypeStruct((1,) + final.shape, f32),
        ),
        in_specs=[pl.BlockSpec(memory_space=pltpu.VMEM)] * 2,
        out_specs=(pl.BlockSpec(memory_space=pl.ANY),) * 2,
        scratch_shapes=[dma((5,))],
        compiler_params=pltpu.CompilerParams(vmem_limit_bytes=8 * 1024 * 1024),
    )(gradient, final)


def solution(mesh):
    placed = (
        P(("groups", "dom"), None, None),
        P(("groups", "shot"), None, "dom", None, None),
        P(("groups", "shot"), None, "dom", None, None),
        P(("groups", "shot"), None, None),
        P(("groups", "shot"), None, None),
        P(("groups", "shot"), None),
    )
    return jax.shard_map(
        functools.partial(per_device, mesh.shape["dom"]),
        mesh=mesh,
        in_specs=placed,
        out_specs=(
            P(("groups", "dom"), "shot", None),
            P(("groups", "shot"), None, "dom", None, None),
        ),
        check_vma=False,
    )
```

```python
import functools

import jax
import jax.numpy as jnp
from jax import lax
from jax.experimental import pallas as pl
from jax.experimental.pallas import tpu as pltpu
from jax.sharding import PartitionSpec as P

ITERS = 4
RADIUS = 6
WIDTH = 4
PAD = 8
CHUNKS = 4
BLOCKS = 4
MESH = pl.DeviceIdType.MESH


def in_hbm(array):
    return pltpu.with_memory_space_constraint(array, pltpu.HBM)

SCALE = 5040.0
CENTRE = 3.0 * -14350.0
OFFSET = (0.0, 8064.0, -1008.0, 128.0, -9.0)


def make_band(band):
    size_y = band.shape[1]
    row = lax.broadcasted_iota(jnp.int32, (2 * size_y, size_y), 0) % size_y
    gap = jnp.abs(row - lax.broadcasted_iota(jnp.int32, (2 * size_y, size_y), 1))
    weights = jnp.zeros(gap.shape, jnp.float32)
    for k in range(1, WIDTH + 1):
        weights = jnp.where(gap == k, OFFSET[k], weights)
    band[...] = weights.astype(jnp.bfloat16)


def stencil(lam, base, later, courant, along, band, far_halo, near_halo):
    planes, size_x, size_y = courant.shape
    rows = size_x // CHUNKS
    zero_row = (lax.axis_index("dom") // lax.axis_size("dom")) * 8

    def lateral(level, first, last):
        for block in range(first, last):
            here = pl.ds(block * WIDTH, WIDTH)
            field = lam[level][here, pl.ds(PAD, size_x), :].reshape(-1, size_y)
            high = field.astype(jnp.bfloat16)
            low = (field - high.astype(jnp.float32)).astype(jnp.bfloat16)
            result = jnp.dot(
                jnp.concatenate([high, low], axis=1), band[...], preferred_element_type=jnp.float32
            )
            along[here, :, :] = result.reshape(WIDTH, size_x, size_y)

    def advance(step, block):
        now = lam[step + 1]
        before = later if step == 3 else lam[step + 2]
        offset = 0 if step == 3 else PAD
        low, high = block * WIDTH, (block + 1) * WIDTH
        for i in range(size_x // 8):
            at = zero_row + i * 8
            here = pl.ds(pl.multiple_of(at, 8), 8)
            padded = pl.ds(pl.multiple_of(at + PAD, 8), 8)
            column = {}
            for q in range(low - WIDTH, high + WIDTH):
                if 0 <= q < planes:
                    column[q] = now[q, padded, :]
                elif q >= planes:
                    column[q] = near_halo[step, WIDTH - 1 - (q - planes), here, :]
            for q in range(low, high):
                centre = column[q]
                total = along[q, here, :] + CENTRE * centre
                for k in range(1, WIDTH + 1):
                    beside = now[q, pl.ds(at + PAD + k, 8), :] + now[q, pl.ds(at + PAD - k, 8), :]
                    beside = beside + column[q + k]
                    if q - k >= 0:
                        beside = beside + column[q - k]
                    total = total + OFFSET[k] * beside
                moved = 2.0 * centre - before[q, pl.ds(pl.multiple_of(at + offset, 8), 8), :]
                scaled = courant[q, here, :] * (1.0 / SCALE)
                lam[step][q, padded, :] = base[step][q, padded, :] + (moved + scaled * total)

    def finish(step, c):
        for i in range(rows // 8):
            at = zero_row + c * rows + i * 8
            here = pl.ds(pl.multiple_of(at, 8), 8)
            padded = pl.ds(pl.multiple_of(at + PAD, 8), 8)
            beyond = [far_halo[step, d, here, :] for d in range(WIDTH)]
            for q in range(WIDTH):
                total = OFFSET[q + 1] * beyond[0]
                for d in range(1, WIDTH - q):
                    total = total + OFFSET[q + 1 + d] * beyond[d]
                scaled = courant[q, here, :] * (1.0 / SCALE)
                lam[step][q, padded, :] = lam[step][q, padded, :] + scaled * total

    return lateral, advance, finish


def backward(
    planes,
    size_x,
    size_y,
    dom_size,
    courant_hbm,
    adjoint_hbm,
    forward_hbm,
    traces_hbm,
    receivers_hbm,
    source_hbm,
    lam0,
    lam1,
    lam2,
    lam3,
    courant,
    forward,
    taper_z,
    taper_xy,
    far_last,
    near_last,
    traces_ref,
    receivers_ref,
    source_ref,
    lam4,
    later,
    along,
    band,
    spots,
    across,
    amounts,
    far_halo,
    near_halo,
    in_sem,
    table_sem,
    far_send,
    far_recv,
    near_send,
    near_recv,
):
    lam = (lam0, lam1, lam2, lam3, lam4)
    dom = lax.axis_index("dom")
    parity = dom % 2
    first_row = dom * planes
    far = dom + 2 * parity - 1
    near = dom + 1 - 2 * parity
    has_far = (far >= 0) & (far < dom_size)
    rows = size_x // CHUNKS

    def depth(q):
        return q + parity * (planes - 1 - 2 * q)

    def load(kind, q):
        z = depth(q)
        if kind == 0:
            source, target = adjoint_hbm.at[0, 1, z], lam4.at[q, pl.ds(PAD, size_x)]
        elif kind == 1:
            source, target = adjoint_hbm.at[0, 0, z], later.at[q]
        elif kind == 2:
            source, target = courant_hbm.at[z], courant.at[q]
        else:
            source, target = forward_hbm.at[0, :, z], forward.at[:, q]
        return pltpu.make_async_copy(source, target, in_sem.at[kind, q])

    barrier = pltpu.get_barrier_semaphore()
    pl.semaphore_signal(barrier, inc=1, device_id={"dom": near}, device_id_type=MESH)

    @pl.when(has_far)
    def _():
        pl.semaphore_signal(barrier, inc=1, device_id={"dom": far}, device_id_type=MESH)

    tables = [
        pltpu.make_async_copy(source, target, table_sem.at[i])
        for i, (source, target) in enumerate(
            ((receivers_hbm, receivers_ref), (traces_hbm, traces_ref), (source_hbm, source_ref))
        )
    ]
    for table in tables:
        table.start()
    order = [0, 1, 2, 3] + list(range(planes - 1, 3, -1))
    for q in order:
        load(0, q).start()

    for level in (1, 2, 3, 4):
        for q in range(planes):
            zero = jnp.zeros((PAD, size_y), jnp.float32)
            lam[level][q, pl.ds(0, PAD), :] = zero
            lam[level][q, pl.ds(PAD + size_x, PAD), :] = zero

    @pl.when(jnp.logical_not(has_far))
    def _():
        far_halo[...] = jnp.zeros(far_halo.shape, jnp.float32)

    make_band(band)

    @pl.when(has_far)
    def _():
        pl.semaphore_wait(barrier, 2)

    @pl.when(jnp.logical_not(has_far))
    def _():
        pl.semaphore_wait(barrier, 1)

    def far_copy(level, c):
        return pltpu.make_async_remote_copy(
            src_ref=lam[level].at[pl.ds(0, WIDTH), pl.ds(PAD + c * rows, rows)],
            dst_ref=far_halo.at[level - 1, :, pl.ds(c * rows, rows)],
            send_sem=far_send.at[level - 1, c],
            recv_sem=far_recv.at[level - 1, c],
            device_id={"dom": far},
            device_id_type=MESH,
        )

    def near_copy(level):
        return pltpu.make_async_remote_copy(
            src_ref=lam[level].at[pl.ds(planes - WIDTH, WIDTH), pl.ds(PAD, size_x)],
            dst_ref=near_halo.at[level - 1],
            send_sem=near_send.at[level - 1],
            recv_sem=near_recv.at[level - 1],
            device_id={"dom": near},
            device_id_type=MESH,
        )

    def far_start(level, c):
        @pl.when(has_far)
        def _():
            far_copy(level, c).start()

    def far_wait(level, c):
        @pl.when(has_far)
        def _():
            far_copy(level, c).wait_recv()

    for q in range(WIDTH):
        load(0, q).wait()
    for c in range(CHUNKS):
        far_start(4, c)
    for q in range(planes - WIDTH, planes):
        load(0, q).wait()
    near_copy(4).start()

    for table in tables[:2]:
        table.wait()
    for kind in (1, 2, 3):
        for q in order:
            load(kind, q).start()

    z_index = receivers_ref[0] - first_row
    z_index = z_index + parity * (planes - 1 - 2 * z_index)
    count = z_index.shape[1]

    def spots_of():
        ids = lax.broadcasted_iota(jnp.int32, (size_x, count), 0)
        across[...] = jnp.where(ids == receivers_ref[1], 1.0, 0.0).astype(jnp.bfloat16)
        for q in range(planes):
            level = jnp.where(z_index == q, 1.0, 0.0).astype(jnp.bfloat16)
            spots[pl.ds(q * size_x, size_x), :] = across[...] * level

    def amounts_of(step):
        value = traces_ref[pl.ds(step, 1), :]
        high = value.astype(jnp.bfloat16).astype(jnp.float32)
        low = value - high
        last = receivers_ref[2]

        def body(i, carry):
            ids = lax.broadcasted_iota(jnp.int32, (16, count), 0) + i * 16
            hit = ids == last
            start = pl.multiple_of(i * 16, 16)
            amounts[step, pl.ds(start, 16), :] = jnp.where(hit, high, 0.0).astype(jnp.bfloat16)
            amounts[step, pl.ds(size_y + start, 16), :] = jnp.where(hit, low, 0.0).astype(jnp.bfloat16)
            return carry

        lax.fori_loop(0, size_y // 16, body, 0)

    def tapers():
        tables[2].wait()
        q_index = lax.broadcasted_iota(jnp.int32, (planes, size_y), 0)
        z_gap = q_index + parity * (planes - 1 - 2 * q_index) + first_row - source_ref[0, 0]
        taper_z[...] = jnp.exp((z_gap * z_gap).astype(jnp.float32) * (-1.0 / (RADIUS * RADIUS)))
        x_gap = lax.broadcasted_iota(jnp.int32, (size_x, size_y), 0) - source_ref[0, 1]
        y_gap = lax.broadcasted_iota(jnp.int32, (size_x, size_y), 1) - source_ref[0, 2]
        square = x_gap * x_gap + y_gap * y_gap
        taper_xy[...] = jnp.exp(square.astype(jnp.float32) * (-1.0 / (RADIUS * RADIUS)))

    spots_of()
    amounts_of(3)


    def inject(step, first, last):
        half = (last - first) * WIDTH // 2
        for part in range(2):
            start = first * WIDTH + part * half
            both = lax.dot_general(
                spots[pl.ds(start * size_x, half * size_x), :],
                amounts[step],
                (((1,), (1,)), ((), ())),
                preferred_element_type=jnp.float32,
            )
            added = both[:, :size_y] + both[:, size_y:]
            lam[step][pl.ds(start, half), pl.ds(PAD, size_x), :] = added.reshape(half, size_x, size_y)

    def advance(step, block):
        now = lam[step + 1]
        before = later if step == 3 else lam[step + 2]
        offset = 0 if step == 3 else PAD
        low, high = block * WIDTH, (block + 1) * WIDTH
        for i in range(size_x // 8):
            at = zero_row + i * 8
            here = pl.ds(pl.multiple_of(at, 8), 8)
            padded = pl.ds(pl.multiple_of(at + PAD, 8), 8)
            column = {}
            for q in range(low - WIDTH, high + WIDTH):
                if 0 <= q < planes:
                    column[q] = now[q, padded, :]
                elif q >= planes:
                    column[q] = near_halo[step, WIDTH - 1 - (q - planes), here, :]
            for q in range(low, high):
                centre = column[q]
                total = along[q, here, :] + CENTRE * centre
                for k in range(1, WIDTH + 1):
                    beside = now[q, pl.ds(at + PAD + k, 8), :] + now[q, pl.ds(at + PAD - k, 8), :]
                    beside = beside + column[q + k]
                    if q - k >= 0:
                        beside = beside + column[q - k]
                    total = total + OFFSET[k] * beside
                moved = 2.0 * centre - before[q, pl.ds(pl.multiple_of(at + offset, 8), 8), :]
                scaled = courant[q, here, :] * (1.0 / SCALE)
                lam[step][q, padded, :] = lam[step][q, padded, :] + (moved + scaled * total)

    lateral, advance, finish = stencil(lam, lam, later, courant, along, band, far_halo, near_halo)

    def wait_near(level):
        near_copy(level).wait_recv()

    def take(step, c):
        far_wait(step + 1, c)
        finish(step, c)
        if step > 0:
            far_start(step, c)

    def edge(step):
        wait_near(step + 1)
        advance(step, 3)
        if step > 0:
            near_copy(step).start()

    inject(3, 0, 4)
    for q in range(WIDTH, planes - WIDTH):
        load(0, q).wait()
    for kind in (1, 2):
        for q in order:
            load(kind, q).wait()
    lateral(4, 0, 4)
    advance(3, 0)
    edge(3)
    take(3, 0)
    advance(3, 2)
    amounts_of(2)
    take(3, 1)
    advance(3, 1)
    amounts_of(1)
    take(3, 2)
    inject(2, 0, 4)
    take(3, 3)

    lateral(3, 0, 4)
    advance(2, 0)
    take(2, 0)
    edge(2)
    advance(2, 2)
    take(2, 1)
    advance(2, 1)
    amounts_of(0)
    take(2, 2)
    inject(1, 0, 4)
    take(2, 3)

    lateral(2, 0, 4)
    advance(1, 0)
    take(1, 0)
    edge(1)
    advance(1, 2)
    take(1, 1)
    inject(0, 0, 4)
    tapers()
    take(1, 2)
    advance(1, 1)
    take(1, 3)

    for q in order:
        load(3, q).wait()
    wait_near(1)
    near_last[0] = near_halo[0]
    for c in range(CHUNKS):
        far_wait(1, c)
    far_last[0] = far_halo[0]
    for level in (1, 2, 3, 4):
        near_copy(level).wait_send()

        @pl.when(has_far)
        def _():
            for c in range(CHUNKS):
                far_copy(level, c).wait_send()


def gradient_of(
    planes,
    size_x,
    size_y,
    base,
    lam1,
    lam2,
    lam3,
    courant,
    forward,
    taper_z,
    taper_xy,
    far_halo,
    near_halo,
    gradient_ref,
    final_ref,
    lam0,
    along,
    band,
    image,
    got_first,
    sent_second,
    got_second,
    first_send,
    first_recv,
    second_send,
    second_recv,
):
    lam = (lam0, lam1, lam2, lam3)
    shot = lax.axis_index("shot")
    parity = lax.axis_index("dom") % 2
    shot_a = shot + 1 - 2 * (shot % 2)
    shot_b = 3 - shot
    shot_c = (shot + 2) % 4

    def depth(q):
        return q + parity * (planes - 1 - 2 * q)

    barrier = pltpu.get_barrier_semaphore()
    for target in (shot_a, shot_b):
        pl.semaphore_signal(barrier, inc=1, device_id={"shot": target}, device_id_type=MESH)

    make_band(band)
    lateral, advance, finish = stencil(lam, (base,), None, courant, along, band, far_halo, near_halo)

    def imaging(block):
        def body(i, carry):
            at = pl.multiple_of(i * 16, 16)
            here = pl.ds(at, 16)
            padded = pl.ds(pl.multiple_of(at + PAD, 8), 16)
            across = taper_xy[here, :]
            for q in range(block * WIDTH, (block + 1) * WIDTH):
                saved = [forward[j, q, here, :].astype(jnp.float32) for j in range(ITERS + 2)]
                total = None
                for step in range(ITERS):
                    accel = saved[step + 2] - 2.0 * saved[step + 1] + saved[step]
                    term = lam[step][q, padded, :] * accel
                    total = term if total is None else total + term
                image[q, here, :] = total * (1.0 - taper_z[pl.ds(q, 1), :] * across)
            return carry

        lax.fori_loop(0, size_x // 16, body, 0)

    piece = size_x // 4

    def first_copy(block, side, which):
        q = block * WIDTH + 2 * side
        target = (shot_a, shot_b)[side]
        part = (target, shot_c)[which]
        return pltpu.make_async_remote_copy(
            src_ref=image.at[pl.ds(q, 2), pl.ds(pl.multiple_of(part * piece, 8), piece)],
            dst_ref=got_first.at[block, side, which],
            send_sem=first_send.at[block, side, which],
            recv_sem=first_recv.at[block, side, which],
            device_id={"shot": target},
            device_id_type=MESH,
        )

    def second_copy(block, side):
        return pltpu.make_async_remote_copy(
            src_ref=sent_second.at[block, side],
            dst_ref=got_second.at[block, side],
            send_sem=second_send.at[block, side],
            recv_sem=second_recv.at[block, side],
            device_id={"shot": (shot_b, shot_a)[side]},
            device_id_type=MESH,
        )

    def reduce_start(block, which):
        for side in range(2):
            first_copy(block, side, which).start()

    def reduce_next(block):
        for side in range(2):
            onward = (shot_b, shot_a)[side]
            q = block * WIDTH + 2 * side
            first_copy(block, side, 1).wait_recv()
            sent_second[block, side] = (
                image[pl.ds(q, 2), pl.ds(pl.multiple_of(onward * piece, 8), piece), :]
                + got_first[block, side, 1]
            )
            second_copy(block, side).start()

    def reduce_end(block):
        for side in range(2):
            first_copy(block, side, 0).wait_recv()
            second_copy(block, side).wait_recv()
            q = block * WIDTH + 2 * side
            own = image[pl.ds(q, 2), pl.ds(pl.multiple_of(shot * piece, 8), piece), :]
            own = own + got_first[block, side, 0] + got_second[block, side]
            for j in range(2):
                gradient_ref[depth(q + j)] = own[j]

    def store(level, block):
        for q in range(block * WIDTH, (block + 1) * WIDTH):
            final_ref[1 - level, depth(q)] = lam[level][q, pl.ds(PAD, size_x), :]

    lateral(1, 0, 4)
    advance(0, 3)
    imaging(3)
    pl.semaphore_wait(barrier, 2)
    reduce_start(3, 1)
    reduce_start(3, 0)
    advance(0, 2)
    imaging(2)
    reduce_start(2, 1)
    reduce_start(2, 0)
    advance(0, 1)
    imaging(1)
    reduce_start(1, 1)
    advance(0, 0)
    for c in range(CHUNKS):
        finish(0, c)
    imaging(0)
    reduce_start(0, 1)
    reduce_start(1, 0)
    reduce_start(0, 0)
    for level in range(2):
        for block in range(BLOCKS):
            store(level, block)
    reduce_next(3)
    reduce_next(2)
    reduce_next(1)
    reduce_next(0)
    reduce_end(3)
    reduce_end(2)
    reduce_end(1)
    for block in range(BLOCKS):
        for side in range(2):
            first_copy(block, side, 0).wait_send()
            first_copy(block, side, 1).wait_send()
            second_copy(block, side).wait_send()
    reduce_end(0)


def write_out(gradient_ref, final_ref, gradient_hbm, final_hbm, sem):
    copies = [pltpu.make_async_copy(gradient_ref, gradient_hbm, sem.at[0])]
    half = final_ref.shape[1] // 2
    for level in range(2):
        for part in range(2):
            at = pl.ds(part * half, half)
            copies.append(
                pltpu.make_async_copy(
                    final_ref.at[level, at], final_hbm.at[0, level, at], sem.at[1 + 2 * level + part]
                )
            )
    for copy in copies:
        copy.start()
    for copy in copies:
        copy.wait()


def per_device(dom_size, courant_sq, adjoint_init, forward_saved, residual_traces, receivers, sources):
    planes, size_x, size_y = courant_sq.shape
    count = receivers.shape[1]
    f32, bf16 = jnp.float32, jnp.bfloat16
    padded = pltpu.VMEM((planes, size_x + 2 * PAD, size_y), f32)
    grid3 = (planes, size_x, size_y)
    dma = pltpu.SemaphoreType.DMA
    piece = (2, size_x // 4, size_y)
    hbm = pl.BlockSpec(memory_space=pltpu.HBM)
    vmem = pl.BlockSpec(memory_space=pltpu.VMEM)
    padded_shape = (planes, size_x + 2 * PAD, size_y)
    halo = (1, WIDTH, size_x, size_y)
    arrays = (
        courant_sq,
        adjoint_init,
        forward_saved,
        residual_traces[0],
        receivers.transpose(2, 0, 1),
        sources,
    )
    done = pl.pallas_call(
        functools.partial(backward, planes, size_x, size_y, dom_size),
        out_shape=tuple(jax.ShapeDtypeStruct(padded_shape, f32) for _ in range(4))
        + (
            jax.ShapeDtypeStruct(grid3, f32),
            jax.ShapeDtypeStruct((ITERS + 2,) + grid3, bf16),
            jax.ShapeDtypeStruct((planes, size_y), f32),
            jax.ShapeDtypeStruct((size_x, size_y), f32),
            jax.ShapeDtypeStruct(halo, f32),
            jax.ShapeDtypeStruct(halo, f32),
        ),
        in_specs=[hbm] * 6,
        out_specs=(vmem,) * 10,
        scratch_shapes=[
            pltpu.VMEM((ITERS, count), f32),
            pltpu.VMEM((3, 1, count), jnp.int32),
            pltpu.SMEM((1, 3), jnp.int32),
            padded,
            pltpu.VMEM(grid3, f32),
            pltpu.VMEM(grid3, f32),
            pltpu.VMEM((2 * size_y, size_y), bf16),
            pltpu.VMEM((planes * size_x, count), bf16),
            pltpu.VMEM((size_x, count), bf16),
            pltpu.VMEM((ITERS, 2 * size_y, count), bf16),
            pltpu.VMEM((ITERS, WIDTH, size_x, size_y), f32),
            pltpu.VMEM((ITERS, WIDTH, size_x, size_y), f32),
            dma((4, planes)),
            dma((3,)),
            dma((ITERS, CHUNKS)),
            dma((ITERS, CHUNKS)),
            dma((ITERS,)),
            dma((ITERS,)),
        ],
        compiler_params=pltpu.CompilerParams(
            collective_id=0, has_side_effects=True, vmem_limit_bytes=28 * 1024 * 1024
        ),
    )(*(in_hbm(array) for array in arrays))
    gradient, final = pl.pallas_call(
        functools.partial(gradient_of, planes, size_x, size_y),
        out_shape=(
            jax.ShapeDtypeStruct((planes, size_x // 4, size_y), f32),
            jax.ShapeDtypeStruct((2, planes, size_x, size_y), f32),
        ),
        in_specs=[vmem] * 10,
        out_specs=(vmem, vmem),
        scratch_shapes=[
            padded,
            pltpu.VMEM(grid3, f32),
            pltpu.VMEM((2 * size_y, size_y), bf16),
            pltpu.VMEM(grid3, f32),
            pltpu.VMEM((BLOCKS, 2, 2) + piece, f32),
            pltpu.VMEM((BLOCKS, 2) + piece, f32),
            pltpu.VMEM((BLOCKS, 2) + piece, f32),
            dma((BLOCKS, 2, 2)),
            dma((BLOCKS, 2, 2)),
            dma((BLOCKS, 2)),
            dma((BLOCKS, 2)),
        ],
        compiler_params=pltpu.CompilerParams(
            collective_id=1, has_side_effects=True, vmem_limit_bytes=20 * 1024 * 1024
        ),
    )(*done)
    return pl.pallas_call(
        write_out,
        out_shape=(
            jax.ShapeDtypeStruct(gradient.shape, f32),
            jax.ShapeDtypeStruct((1,) + final.shape, f32),
        ),
        in_specs=[pl.BlockSpec(memory_space=pltpu.VMEM)] * 2,
        out_specs=(pl.BlockSpec(memory_space=pl.ANY),) * 2,
        scratch_shapes=[dma((5,))],
        compiler_params=pltpu.CompilerParams(vmem_limit_bytes=8 * 1024 * 1024),
    )(gradient, final)


def solution(mesh):
    placed = (
        P(("groups", "dom"), None, None),
        P(("groups", "shot"), None, "dom", None, None),
        P(("groups", "shot"), None, "dom", None, None),
        P(("groups", "shot"), None, None),
        P(("groups", "shot"), None, None),
        P(("groups", "shot"), None),
    )
    return jax.shard_map(
        functools.partial(per_device, mesh.shape["dom"]),
        mesh=mesh,
        in_specs=placed,
        out_specs=(
            P(("groups", "dom"), "shot", None),
            P(("groups", "shot"), None, "dom", None, None),
        ),
        check_vma=False,
    )
```

```python
import functools

import jax
import jax.numpy as jnp
from jax import lax
from jax.experimental import pallas as pl
from jax.experimental.pallas import tpu as pltpu
from jax.sharding import PartitionSpec as P

ITERS = 4
RADIUS = 6
WIDTH = 4
PAD = 8
CHUNKS = 4
BLOCKS = 4
MESH = pl.DeviceIdType.MESH


def in_hbm(array):
    return pltpu.with_memory_space_constraint(array, pltpu.HBM)

SCALE = 5040.0
CENTRE = 3.0 * -14350.0
OFFSET = (0.0, 8064.0, -1008.0, 128.0, -9.0)


def kernel(
    planes,
    size_x,
    size_y,
    dom_size,
    courant_hbm,
    adjoint_hbm,
    forward_hbm,
    traces_hbm,
    receivers_hbm,
    source_hbm,
    gradient_ref,
    final_ref,
    traces_ref,
    receivers_ref,
    source_ref,
    lam0,
    lam1,
    lam2,
    lam3,
    lam4,
    later,
    courant,
    forward,
    along,
    band,
    spots,
    across,
    amounts,
    image,
    taper_z,
    taper_xy,
    far_halo,
    near_halo,
    got_first,
    sent_second,
    got_second,
    in_sem,
    table_sem,
    far_send,
    far_recv,
    near_send,
    near_recv,
    first_send,
    first_recv,
    second_send,
    second_recv,
):
    lam = (lam0, lam1, lam2, lam3, lam4)
    dom = lax.axis_index("dom")
    shot = lax.axis_index("shot")
    parity = dom % 2
    first_row = dom * planes
    far = dom + 2 * parity - 1
    near = dom + 1 - 2 * parity
    has_far = (far >= 0) & (far < dom_size)
    shot_a = shot + 1 - 2 * (shot % 2)
    shot_b = 3 - shot
    shot_c = (shot + 2) % 4
    rows = size_x // CHUNKS
    zero_row = (dom // dom_size) * 8

    def depth(q):
        return q + parity * (planes - 1 - 2 * q)

    def load(kind, q):
        z = depth(q)
        if kind == 0:
            source, target = adjoint_hbm.at[0, 1, z], lam4.at[q, pl.ds(PAD, size_x)]
        elif kind == 1:
            source, target = adjoint_hbm.at[0, 0, z], later.at[q]
        elif kind == 2:
            source, target = courant_hbm.at[z], courant.at[q]
        else:
            source, target = forward_hbm.at[0, :, z], forward.at[:, q]
        return pltpu.make_async_copy(source, target, in_sem.at[kind, q])

    barrier = pltpu.get_barrier_semaphore()
    for axis, target in (("dom", near), ("shot", shot_a), ("shot", shot_b)):
        pl.semaphore_signal(barrier, inc=1, device_id={axis: target}, device_id_type=MESH)

    @pl.when(has_far)
    def _():
        pl.semaphore_signal(barrier, inc=1, device_id={"dom": far}, device_id_type=MESH)

    tables = [
        pltpu.make_async_copy(source, target, table_sem.at[i])
        for i, (source, target) in enumerate(
            ((receivers_hbm, receivers_ref), (traces_hbm, traces_ref), (source_hbm, source_ref))
        )
    ]
    for table in tables:
        table.start()
    order = [0, 1, 2, 3] + list(range(planes - 1, 3, -1))
    for q in order:
        load(0, q).start()

    for level in (1, 2, 3, 4):
        for q in range(planes):
            zero = jnp.zeros((PAD, size_y), jnp.float32)
            lam[level][q, pl.ds(0, PAD), :] = zero
            lam[level][q, pl.ds(PAD + size_x, PAD), :] = zero

    @pl.when(jnp.logical_not(has_far))
    def _():
        far_halo[...] = jnp.zeros(far_halo.shape, jnp.float32)

    row = lax.broadcasted_iota(jnp.int32, (2 * size_y, size_y), 0) % size_y
    gap = jnp.abs(row - lax.broadcasted_iota(jnp.int32, (2 * size_y, size_y), 1))
    weights = jnp.zeros(gap.shape, jnp.float32)
    for k in range(1, WIDTH + 1):
        weights = jnp.where(gap == k, OFFSET[k], weights)
    band[...] = weights.astype(jnp.bfloat16)

    def far_copy(level, c):
        return pltpu.make_async_remote_copy(
            src_ref=lam[level].at[pl.ds(0, WIDTH), pl.ds(PAD + c * rows, rows)],
            dst_ref=far_halo.at[level - 1, :, pl.ds(c * rows, rows)],
            send_sem=far_send.at[level - 1, c],
            recv_sem=far_recv.at[level - 1, c],
            device_id={"dom": far},
            device_id_type=MESH,
        )

    def near_copy(level):
        return pltpu.make_async_remote_copy(
            src_ref=lam[level].at[pl.ds(planes - WIDTH, WIDTH), pl.ds(PAD, size_x)],
            dst_ref=near_halo.at[level - 1],
            send_sem=near_send.at[level - 1],
            recv_sem=near_recv.at[level - 1],
            device_id={"dom": near},
            device_id_type=MESH,
        )

    def far_start(level, c):
        @pl.when(has_far)
        def _():
            far_copy(level, c).start()

    def far_wait(level, c):
        @pl.when(has_far)
        def _():
            far_copy(level, c).wait_recv()


    for table in tables[:2]:
        table.wait()
    for kind in (1, 2, 3):
        for q in order:
            load(kind, q).start()

    z_index = receivers_ref[0] - first_row
    z_index = z_index + parity * (planes - 1 - 2 * z_index)
    count = z_index.shape[1]

    def spots_of():
        ids = lax.broadcasted_iota(jnp.int32, (size_x, count), 0)
        across[...] = jnp.where(ids == receivers_ref[1], 1.0, 0.0).astype(jnp.bfloat16)
        for q in range(planes):
            level = jnp.where(z_index == q, 1.0, 0.0).astype(jnp.bfloat16)
            spots[pl.ds(q * size_x, size_x), :] = across[...] * level

    def amounts_of(step):
        value = traces_ref[pl.ds(step, 1), :]
        high = value.astype(jnp.bfloat16).astype(jnp.float32)
        low = value - high
        last = receivers_ref[2]

        def body(i, carry):
            ids = lax.broadcasted_iota(jnp.int32, (16, count), 0) + i * 16
            hit = ids == last
            start = pl.multiple_of(i * 16, 16)
            amounts[step, pl.ds(start, 16), :] = jnp.where(hit, high, 0.0).astype(jnp.bfloat16)
            amounts[step, pl.ds(size_y + start, 16), :] = jnp.where(hit, low, 0.0).astype(jnp.bfloat16)
            return carry

        lax.fori_loop(0, size_y // 16, body, 0)

    def tapers():
        tables[2].wait()
        q_index = lax.broadcasted_iota(jnp.int32, (planes, size_y), 0)
        z_gap = q_index + parity * (planes - 1 - 2 * q_index) + first_row - source_ref[0, 0]
        taper_z[...] = jnp.exp((z_gap * z_gap).astype(jnp.float32) * (-1.0 / (RADIUS * RADIUS)))
        x_gap = lax.broadcasted_iota(jnp.int32, (size_x, size_y), 0) - source_ref[0, 1]
        y_gap = lax.broadcasted_iota(jnp.int32, (size_x, size_y), 1) - source_ref[0, 2]
        square = x_gap * x_gap + y_gap * y_gap
        taper_xy[...] = jnp.exp(square.astype(jnp.float32) * (-1.0 / (RADIUS * RADIUS)))

    spots_of()
    amounts_of(3)


    def inject(step, first, last):
        half = (last - first) * WIDTH // 2
        for part in range(2):
            start = first * WIDTH + part * half
            both = lax.dot_general(
                spots[pl.ds(start * size_x, half * size_x), :],
                amounts[step],
                (((1,), (1,)), ((), ())),
                preferred_element_type=jnp.float32,
            )
            added = both[:, :size_y] + both[:, size_y:]
            lam[step][pl.ds(start, half), pl.ds(PAD, size_x), :] = added.reshape(half, size_x, size_y)

    def lateral(level, first, last):
        for block in range(first, last):
            here = pl.ds(block * WIDTH, WIDTH)
            field = lam[level][here, pl.ds(PAD, size_x), :].reshape(-1, size_y)
            high = field.astype(jnp.bfloat16)
            low = (field - high.astype(jnp.float32)).astype(jnp.bfloat16)
            result = jnp.dot(
                jnp.concatenate([high, low], axis=1), band[...], preferred_element_type=jnp.float32
            )
            along[here, :, :] = result.reshape(WIDTH, size_x, size_y)

    def advance(step, block):
        now = lam[step + 1]
        before = later if step == 3 else lam[step + 2]
        offset = 0 if step == 3 else PAD
        low, high = block * WIDTH, (block + 1) * WIDTH
        for i in range(size_x // 8):
            at = zero_row + i * 8
            here = pl.ds(pl.multiple_of(at, 8), 8)
            padded = pl.ds(pl.multiple_of(at + PAD, 8), 8)
            column = {}
            for q in range(low - WIDTH, high + WIDTH):
                if 0 <= q < planes:
                    column[q] = now[q, padded, :]
                elif q >= planes:
                    column[q] = near_halo[step, WIDTH - 1 - (q - planes), here, :]
            for q in range(low, high):
                centre = column[q]
                total = along[q, here, :] + CENTRE * centre
                for k in range(1, WIDTH + 1):
                    beside = now[q, pl.ds(at + PAD + k, 8), :] + now[q, pl.ds(at + PAD - k, 8), :]
                    beside = beside + column[q + k]
                    if q - k >= 0:
                        beside = beside + column[q - k]
                    total = total + OFFSET[k] * beside
                moved = 2.0 * centre - before[q, pl.ds(pl.multiple_of(at + offset, 8), 8), :]
                scaled = courant[q, here, :] * (1.0 / SCALE)
                lam[step][q, padded, :] = lam[step][q, padded, :] + (moved + scaled * total)

    def finish(step, c):
        for i in range(rows // 8):
            at = zero_row + c * rows + i * 8
            here = pl.ds(pl.multiple_of(at, 8), 8)
            padded = pl.ds(pl.multiple_of(at + PAD, 8), 8)
            beyond = [far_halo[step, d, here, :] for d in range(WIDTH)]
            for q in range(WIDTH):
                total = OFFSET[q + 1] * beyond[0]
                for d in range(1, WIDTH - q):
                    total = total + OFFSET[q + 1 + d] * beyond[d]
                scaled = courant[q, here, :] * (1.0 / SCALE)
                lam[step][q, padded, :] = lam[step][q, padded, :] + scaled * total

    def imaging(block):
        def body(i, carry):
            at = pl.multiple_of(i * 16, 16)
            here = pl.ds(at, 16)
            padded = pl.ds(pl.multiple_of(at + PAD, 8), 16)
            across = taper_xy[here, :]
            for q in range(block * WIDTH, (block + 1) * WIDTH):
                saved = [forward[j, q, here, :].astype(jnp.float32) for j in range(ITERS + 2)]
                total = None
                for step in range(ITERS):
                    accel = saved[step + 2] - 2.0 * saved[step + 1] + saved[step]
                    term = lam[step][q, padded, :] * accel
                    total = term if total is None else total + term
                image[q, here, :] = total * (1.0 - taper_z[pl.ds(q, 1), :] * across)
            return carry

        lax.fori_loop(0, size_x // 16, body, 0)

    piece = size_x // 4

    def first_copy(block, side, which):
        q = block * WIDTH + 2 * side
        target = (shot_a, shot_b)[side]
        part = (target, shot_c)[which]
        return pltpu.make_async_remote_copy(
            src_ref=image.at[pl.ds(q, 2), pl.ds(pl.multiple_of(part * piece, 8), piece)],
            dst_ref=got_first.at[block, side, which],
            send_sem=first_send.at[block, side, which],
            recv_sem=first_recv.at[block, side, which],
            device_id={"shot": target},
            device_id_type=MESH,
        )

    def second_copy(block, side):
        return pltpu.make_async_remote_copy(
            src_ref=sent_second.at[block, side],
            dst_ref=got_second.at[block, side],
            send_sem=second_send.at[block, side],
            recv_sem=second_recv.at[block, side],
            device_id={"shot": (shot_b, shot_a)[side]},
            device_id_type=MESH,
        )

    def reduce_start(block, which):
        for side in range(2):
            first_copy(block, side, which).start()

    def reduce_next(block):
        for side in range(2):
            onward = (shot_b, shot_a)[side]
            q = block * WIDTH + 2 * side
            first_copy(block, side, 1).wait_recv()
            sent_second[block, side] = (
                image[pl.ds(q, 2), pl.ds(pl.multiple_of(onward * piece, 8), piece), :]
                + got_first[block, side, 1]
            )
            second_copy(block, side).start()

    def reduce_end(block):
        for side in range(2):
            first_copy(block, side, 0).wait_recv()
            second_copy(block, side).wait_recv()
            q = block * WIDTH + 2 * side
            own = image[pl.ds(q, 2), pl.ds(pl.multiple_of(shot * piece, 8), piece), :]
            own = own + got_first[block, side, 0] + got_second[block, side]
            for j in range(2):
                gradient_ref[depth(q + j)] = own[j]

    def store(level, block):
        for q in range(block * WIDTH, (block + 1) * WIDTH):
            final_ref[1 - level, depth(q)] = lam[level][q, pl.ds(PAD, size_x), :]

    def wait_near(level):
        near_copy(level).wait_recv()

    def take(step, c):
        far_wait(step + 1, c)
        finish(step, c)
        if step > 0:
            far_start(step, c)

    def edge(step):
        wait_near(step + 1)
        advance(step, 3)
        if step > 0:
            near_copy(step).start()

    amounts_of(2)
    amounts_of(1)
    amounts_of(0)
    inject(3, 0, 4)
    for q in order:
        load(0, q).wait()
    for kind in (1, 2):
        for q in order:
            load(kind, q).wait()
    lateral(4, 0, 4)
    advance(3, 0)
    advance(3, 2)
    advance(3, 1)
    inject(2, 0, 4)

    @pl.when(has_far)
    def _():
        pl.semaphore_wait(barrier, 4)

    @pl.when(jnp.logical_not(has_far))
    def _():
        pl.semaphore_wait(barrier, 3)

    for c in range(CHUNKS):
        far_start(4, c)
    near_copy(4).start()
    inject(1, 0, 4)
    for c in range(CHUNKS):
        take(3, c)

    lateral(3, 0, 3)
    advance(2, 0)
    advance(2, 1)
    edge(3)
    take(2, 0)
    lateral(3, 3, 4)
    advance(2, 2)
    take(2, 1)
    edge(2)
    take(2, 2)
    take(2, 3)

    lateral(2, 0, 4)
    advance(1, 0)
    take(1, 0)
    advance(1, 1)
    take(1, 1)
    advance(1, 2)
    inject(0, 2, 4)
    edge(1)
    take(1, 2)
    take(1, 3)

    lateral(1, 2, 4)
    edge(0)
    tapers()
    for q in order:
        load(3, q).wait()
    imaging(3)
    reduce_start(3, 1)
    reduce_start(3, 0)
    inject(0, 0, 2)
    lateral(1, 0, 2)
    advance(0, 2)
    imaging(2)
    reduce_start(2, 1)
    reduce_start(2, 0)
    advance(0, 0)
    take(0, 0)
    advance(0, 1)
    imaging(1)
    reduce_start(1, 1)
    take(0, 1)
    for block in range(BLOCKS):
        store(1, block)
    for block in range(1, BLOCKS):
        store(0, block)
    take(0, 2)
    reduce_next(3)
    take(0, 3)
    imaging(0)
    reduce_start(0, 1)
    reduce_start(1, 0)
    reduce_start(0, 0)
    store(0, 0)
    reduce_next(2)
    reduce_next(1)
    for level in (1, 2, 3, 4):
        near_copy(level).wait_send()

        @pl.when(has_far)
        def _():
            for c in range(CHUNKS):
                far_copy(level, c).wait_send()

    reduce_next(0)
    reduce_end(3)
    reduce_end(2)
    reduce_end(1)
    for block in range(BLOCKS):
        for side in range(2):
            first_copy(block, side, 0).wait_send()
            first_copy(block, side, 1).wait_send()
            second_copy(block, side).wait_send()
    reduce_end(0)


def write_out(gradient_ref, final_ref, gradient_hbm, final_hbm, sem):
    copies = [pltpu.make_async_copy(gradient_ref, gradient_hbm, sem.at[0])]
    half = final_ref.shape[1] // 2
    for level in range(2):
        for part in range(2):
            at = pl.ds(part * half, half)
            copies.append(
                pltpu.make_async_copy(
                    final_ref.at[level, at], final_hbm.at[0, level, at], sem.at[1 + 2 * level + part]
                )
            )
    for copy in copies:
        copy.start()
    for copy in copies:
        copy.wait()


def per_device(dom_size, courant_sq, adjoint_init, forward_saved, residual_traces, receivers, sources):
    planes, size_x, size_y = courant_sq.shape
    count = receivers.shape[1]
    f32, bf16 = jnp.float32, jnp.bfloat16
    padded = pltpu.VMEM((planes, size_x + 2 * PAD, size_y), f32)
    grid3 = (planes, size_x, size_y)
    dma = pltpu.SemaphoreType.DMA
    piece = (2, size_x // 4, size_y)
    gradient, final = pl.pallas_call(
        functools.partial(kernel, planes, size_x, size_y, dom_size),
        out_shape=(
            jax.ShapeDtypeStruct((planes, size_x // 4, size_y), f32),
            jax.ShapeDtypeStruct((2, planes, size_x, size_y), f32),
        ),
        in_specs=[pl.BlockSpec(memory_space=pltpu.HBM)] * 6,
        out_specs=(pl.BlockSpec(memory_space=pltpu.VMEM), pl.BlockSpec(memory_space=pltpu.VMEM)),
        scratch_shapes=[
            pltpu.VMEM((ITERS, count), f32),
            pltpu.VMEM((3, 1, count), jnp.int32),
            pltpu.SMEM((1, 3), jnp.int32),
        ]
        + [padded] * 5
        + [
            pltpu.VMEM(grid3, f32),
            pltpu.VMEM(grid3, f32),
            pltpu.VMEM((ITERS + 2,) + grid3, bf16),
            pltpu.VMEM(grid3, f32),
            pltpu.VMEM((2 * size_y, size_y), bf16),
            pltpu.VMEM((planes * size_x, count), bf16),
            pltpu.VMEM((size_x, count), bf16),
            pltpu.VMEM((ITERS, 2 * size_y, count), bf16),
            pltpu.VMEM(grid3, f32),
            pltpu.VMEM((planes, size_y), f32),
            pltpu.VMEM((size_x, size_y), f32),
            pltpu.VMEM((ITERS, WIDTH, size_x, size_y), f32),
            pltpu.VMEM((ITERS, WIDTH, size_x, size_y), f32),
            pltpu.VMEM((BLOCKS, 2, 2) + piece, f32),
            pltpu.VMEM((BLOCKS, 2) + piece, f32),
            pltpu.VMEM((BLOCKS, 2) + piece, f32),
            dma((4, planes)),
            dma((3,)),
            dma((ITERS, CHUNKS)),
            dma((ITERS, CHUNKS)),
            dma((ITERS,)),
            dma((ITERS,)),
            dma((BLOCKS, 2, 2)),
            dma((BLOCKS, 2, 2)),
            dma((BLOCKS, 2)),
            dma((BLOCKS, 2)),
        ],
        compiler_params=pltpu.CompilerParams(
            collective_id=0, has_side_effects=True, vmem_limit_bytes=34 * 1024 * 1024
        ),
    )(
        *(
            in_hbm(array)
            for array in (
                courant_sq,
                adjoint_init,
                forward_saved,
                residual_traces[0],
                receivers.transpose(2, 0, 1),
                sources,
            )
        )
    )
    return pl.pallas_call(
        write_out,
        out_shape=(
            jax.ShapeDtypeStruct(gradient.shape, f32),
            jax.ShapeDtypeStruct((1,) + final.shape, f32),
        ),
        in_specs=[pl.BlockSpec(memory_space=pltpu.VMEM)] * 2,
        out_specs=(pl.BlockSpec(memory_space=pl.ANY),) * 2,
        scratch_shapes=[dma((5,))],
        compiler_params=pltpu.CompilerParams(vmem_limit_bytes=8 * 1024 * 1024),
    )(gradient, final)


def solution(mesh):
    placed = (
        P(("groups", "dom"), None, None),
        P(("groups", "shot"), None, "dom", None, None),
        P(("groups", "shot"), None, "dom", None, None),
        P(("groups", "shot"), None, None),
        P(("groups", "shot"), None, None),
        P(("groups", "shot"), None),
    )
    return jax.shard_map(
        functools.partial(per_device, mesh.shape["dom"]),
        mesh=mesh,
        in_specs=placed,
        out_specs=(
            P(("groups", "dom"), "shot", None),
            P(("groups", "shot"), None, "dom", None, None),
        ),
        check_vma=False,
    )
```

```python
import functools

import jax
import jax.numpy as jnp
from jax import lax
from jax.experimental import pallas as pl
from jax.experimental.pallas import tpu as pltpu
from jax.sharding import PartitionSpec as P

ITERS = 4
RADIUS = 6
WIDTH = 4
PAD = 8
CHUNKS = 4
BLOCKS = 4
MESH = pl.DeviceIdType.MESH


def in_hbm(array):
    return pltpu.with_memory_space_constraint(array, pltpu.HBM)

SCALE = 5040.0
CENTRE = 3.0 * -14350.0
OFFSET = (0.0, 8064.0, -1008.0, 128.0, -9.0)


def kernel(
    planes,
    size_x,
    size_y,
    dom_size,
    courant_hbm,
    adjoint_hbm,
    forward_hbm,
    traces_hbm,
    receivers_hbm,
    source_hbm,
    gradient_ref,
    final_ref,
    traces_ref,
    receivers_ref,
    source_ref,
    lam0,
    lam1,
    lam2,
    lam3,
    lam4,
    later,
    courant,
    forward,
    along,
    band,
    spots,
    across,
    amounts,
    image,
    taper_z,
    taper_xy,
    far_halo,
    near_halo,
    got_first,
    sent_second,
    got_second,
    in_sem,
    table_sem,
    far_send,
    far_recv,
    near_send,
    near_recv,
    first_send,
    first_recv,
    second_send,
    second_recv,
):
    lam = (lam0, lam1, lam2, lam3, lam4)
    dom = lax.axis_index("dom")
    shot = lax.axis_index("shot")
    parity = dom % 2
    first_row = dom * planes
    far = dom + 2 * parity - 1
    near = dom + 1 - 2 * parity
    has_far = (far >= 0) & (far < dom_size)
    shot_a = shot + 1 - 2 * (shot % 2)
    shot_b = 3 - shot
    shot_c = (shot + 2) % 4
    rows = size_x // CHUNKS
    zero_row = (dom // dom_size) * 8

    def depth(q):
        return q + parity * (planes - 1 - 2 * q)

    def load(kind, q):
        z = depth(q)
        if kind == 0:
            source, target = adjoint_hbm.at[0, 1, z], lam4.at[q, pl.ds(PAD, size_x)]
        elif kind == 1:
            source, target = adjoint_hbm.at[0, 0, z], later.at[q]
        elif kind == 2:
            source, target = courant_hbm.at[z], courant.at[q]
        else:
            source, target = forward_hbm.at[0, :, z], forward.at[:, q]
        return pltpu.make_async_copy(source, target, in_sem.at[kind, q])

    barrier = pltpu.get_barrier_semaphore()
    for axis, target in (("dom", near), ("shot", shot_a), ("shot", shot_b)):
        pl.semaphore_signal(barrier, inc=1, device_id={axis: target}, device_id_type=MESH)

    @pl.when(has_far)
    def _():
        pl.semaphore_signal(barrier, inc=1, device_id={"dom": far}, device_id_type=MESH)

    tables = [
        pltpu.make_async_copy(source, target, table_sem.at[i])
        for i, (source, target) in enumerate(
            ((receivers_hbm, receivers_ref), (traces_hbm, traces_ref), (source_hbm, source_ref))
        )
    ]
    for table in tables:
        table.start()
    order = [0, 1, 2, 3] + list(range(planes - 1, 3, -1))
    for q in order:
        load(0, q).start()

    for level in (1, 2, 3, 4):
        for q in range(planes):
            zero = jnp.zeros((PAD, size_y), jnp.float32)
            lam[level][q, pl.ds(0, PAD), :] = zero
            lam[level][q, pl.ds(PAD + size_x, PAD), :] = zero

    @pl.when(jnp.logical_not(has_far))
    def _():
        far_halo[...] = jnp.zeros(far_halo.shape, jnp.float32)

    row = lax.broadcasted_iota(jnp.int32, (2 * size_y, size_y), 0) % size_y
    gap = jnp.abs(row - lax.broadcasted_iota(jnp.int32, (2 * size_y, size_y), 1))
    weights = jnp.zeros(gap.shape, jnp.float32)
    for k in range(1, WIDTH + 1):
        weights = jnp.where(gap == k, OFFSET[k], weights)
    band[...] = weights.astype(jnp.bfloat16)

    def far_copy(level, c):
        return pltpu.make_async_remote_copy(
            src_ref=lam[level].at[pl.ds(0, WIDTH), pl.ds(PAD + c * rows, rows)],
            dst_ref=far_halo.at[level - 1, :, pl.ds(c * rows, rows)],
            send_sem=far_send.at[level - 1, c],
            recv_sem=far_recv.at[level - 1, c],
            device_id={"dom": far},
            device_id_type=MESH,
        )

    def near_copy(level):
        return pltpu.make_async_remote_copy(
            src_ref=lam[level].at[pl.ds(planes - WIDTH, WIDTH), pl.ds(PAD, size_x)],
            dst_ref=near_halo.at[level - 1],
            send_sem=near_send.at[level - 1],
            recv_sem=near_recv.at[level - 1],
            device_id={"dom": near},
            device_id_type=MESH,
        )

    def far_start(level, c):
        @pl.when(has_far)
        def _():
            far_copy(level, c).start()

    def far_wait(level, c):
        @pl.when(has_far)
        def _():
            far_copy(level, c).wait_recv()


    for table in tables[:2]:
        table.wait()
    for kind in (1, 2, 3):
        for q in order:
            load(kind, q).start()

    z_index = receivers_ref[0] - first_row
    z_index = z_index + parity * (planes - 1 - 2 * z_index)
    count = z_index.shape[1]

    def spots_of():
        ids = lax.broadcasted_iota(jnp.int32, (size_x, count), 0)
        across[...] = jnp.where(ids == receivers_ref[1], 1.0, 0.0).astype(jnp.bfloat16)
        for q in range(planes):
            level = jnp.where(z_index == q, 1.0, 0.0).astype(jnp.bfloat16)
            spots[pl.ds(q * size_x, size_x), :] = across[...] * level

    def amounts_of(step):
        value = traces_ref[pl.ds(step, 1), :]
        high = value.astype(jnp.bfloat16).astype(jnp.float32)
        low = value - high
        last = receivers_ref[2]

        def body(i, carry):
            ids = lax.broadcasted_iota(jnp.int32, (16, count), 0) + i * 16
            hit = ids == last
            start = pl.multiple_of(i * 16, 16)
            amounts[step, pl.ds(start, 16), :] = jnp.where(hit, high, 0.0).astype(jnp.bfloat16)
            amounts[step, pl.ds(size_y + start, 16), :] = jnp.where(hit, low, 0.0).astype(jnp.bfloat16)
            return carry

        lax.fori_loop(0, size_y // 16, body, 0)

    def tapers():
        tables[2].wait()
        q_index = lax.broadcasted_iota(jnp.int32, (planes, size_y), 0)
        z_gap = q_index + parity * (planes - 1 - 2 * q_index) + first_row - source_ref[0, 0]
        taper_z[...] = jnp.exp((z_gap * z_gap).astype(jnp.float32) * (-1.0 / (RADIUS * RADIUS)))
        x_gap = lax.broadcasted_iota(jnp.int32, (size_x, size_y), 0) - source_ref[0, 1]
        y_gap = lax.broadcasted_iota(jnp.int32, (size_x, size_y), 1) - source_ref[0, 2]
        square = x_gap * x_gap + y_gap * y_gap
        taper_xy[...] = jnp.exp(square.astype(jnp.float32) * (-1.0 / (RADIUS * RADIUS)))

    spots_of()
    amounts_of(3)


    def inject(step, first, last):
        half = (last - first) * WIDTH // 2
        for part in range(2):
            start = first * WIDTH + part * half
            both = lax.dot_general(
                spots[pl.ds(start * size_x, half * size_x), :],
                amounts[step],
                (((1,), (1,)), ((), ())),
                preferred_element_type=jnp.float32,
            )
            added = both[:, :size_y] + both[:, size_y:]
            lam[step][pl.ds(start, half), pl.ds(PAD, size_x), :] = added.reshape(half, size_x, size_y)

    def lateral(level, first, last):
        for block in range(first, last):
            here = pl.ds(block * WIDTH, WIDTH)
            field = lam[level][here, pl.ds(PAD, size_x), :].reshape(-1, size_y)
            high = field.astype(jnp.bfloat16)
            low = (field - high.astype(jnp.float32)).astype(jnp.bfloat16)
            result = jnp.dot(
                jnp.concatenate([high, low], axis=1), band[...], preferred_element_type=jnp.float32
            )
            along[here, :, :] = result.reshape(WIDTH, size_x, size_y)

    def advance(step, block):
        now = lam[step + 1]
        before = later if step == 3 else lam[step + 2]
        offset = 0 if step == 3 else PAD
        low, high = block * WIDTH, (block + 1) * WIDTH
        for i in range(size_x // 8):
            at = zero_row + i * 8
            here = pl.ds(pl.multiple_of(at, 8), 8)
            padded = pl.ds(pl.multiple_of(at + PAD, 8), 8)
            column = {}
            for q in range(low - WIDTH, high + WIDTH):
                if 0 <= q < planes:
                    column[q] = now[q, padded, :]
                elif q >= planes:
                    column[q] = near_halo[step, WIDTH - 1 - (q - planes), here, :]
            for q in range(low, high):
                centre = column[q]
                total = along[q, here, :] + CENTRE * centre
                for k in range(1, WIDTH + 1):
                    beside = now[q, pl.ds(at + PAD + k, 8), :] + now[q, pl.ds(at + PAD - k, 8), :]
                    beside = beside + column[q + k]
                    if q - k >= 0:
                        beside = beside + column[q - k]
                    total = total + OFFSET[k] * beside
                moved = 2.0 * centre - before[q, pl.ds(pl.multiple_of(at + offset, 8), 8), :]
                scaled = courant[q, here, :] * (1.0 / SCALE)
                lam[step][q, padded, :] = lam[step][q, padded, :] + (moved + scaled * total)

    def finish(step, c):
        for i in range(rows // 8):
            at = zero_row + c * rows + i * 8
            here = pl.ds(pl.multiple_of(at, 8), 8)
            padded = pl.ds(pl.multiple_of(at + PAD, 8), 8)
            beyond = [far_halo[step, d, here, :] for d in range(WIDTH)]
            for q in range(WIDTH):
                total = OFFSET[q + 1] * beyond[0]
                for d in range(1, WIDTH - q):
                    total = total + OFFSET[q + 1 + d] * beyond[d]
                scaled = courant[q, here, :] * (1.0 / SCALE)
                lam[step][q, padded, :] = lam[step][q, padded, :] + scaled * total

    def imaging(block):
        def body(i, carry):
            at = pl.multiple_of(i * 16, 16)
            here = pl.ds(at, 16)
            padded = pl.ds(pl.multiple_of(at + PAD, 8), 16)
            across = taper_xy[here, :]
            for q in range(block * WIDTH, (block + 1) * WIDTH):
                saved = [forward[j, q, here, :].astype(jnp.float32) for j in range(ITERS + 2)]
                total = None
                for step in range(ITERS):
                    accel = saved[step + 2] - 2.0 * saved[step + 1] + saved[step]
                    term = lam[step][q, padded, :] * accel
                    total = term if total is None else total + term
                image[q, here, :] = total * (1.0 - taper_z[pl.ds(q, 1), :] * across)
            return carry

        lax.fori_loop(0, size_x // 16, body, 0)

    piece = size_x // 4

    def first_copy(block, side, which):
        q = block * WIDTH + 2 * side
        target = (shot_a, shot_b)[side]
        part = (target, shot_c)[which]
        return pltpu.make_async_remote_copy(
            src_ref=image.at[pl.ds(q, 2), pl.ds(pl.multiple_of(part * piece, 8), piece)],
            dst_ref=got_first.at[block, side, which],
            send_sem=first_send.at[block, side, which],
            recv_sem=first_recv.at[block, side, which],
            device_id={"shot": target},
            device_id_type=MESH,
        )

    def second_copy(block, side):
        return pltpu.make_async_remote_copy(
            src_ref=sent_second.at[block, side],
            dst_ref=got_second.at[block, side],
            send_sem=second_send.at[block, side],
            recv_sem=second_recv.at[block, side],
            device_id={"shot": (shot_b, shot_a)[side]},
            device_id_type=MESH,
        )

    def reduce_start(block, which):
        for side in range(2):
            first_copy(block, side, which).start()

    def reduce_next(block):
        for side in range(2):
            onward = (shot_b, shot_a)[side]
            q = block * WIDTH + 2 * side
            first_copy(block, side, 1).wait_recv()
            sent_second[block, side] = (
                image[pl.ds(q, 2), pl.ds(pl.multiple_of(onward * piece, 8), piece), :]
                + got_first[block, side, 1]
            )
            second_copy(block, side).start()

    def reduce_end(block):
        for side in range(2):
            first_copy(block, side, 0).wait_recv()
            second_copy(block, side).wait_recv()
            q = block * WIDTH + 2 * side
            own = image[pl.ds(q, 2), pl.ds(pl.multiple_of(shot * piece, 8), piece), :]
            own = own + got_first[block, side, 0] + got_second[block, side]
            for j in range(2):
                gradient_ref[depth(q + j)] = own[j]

    def store(level, block):
        for q in range(block * WIDTH, (block + 1) * WIDTH):
            final_ref[1 - level, depth(q)] = lam[level][q, pl.ds(PAD, size_x), :]

    def wait_near(level):
        near_copy(level).wait_recv()

    def take(step, c):
        far_wait(step + 1, c)
        finish(step, c)
        if step > 0:
            far_start(step, c)

    def edge(step):
        wait_near(step + 1)
        advance(step, 3)
        if step > 0:
            near_copy(step).start()

    amounts_of(2)
    amounts_of(1)
    amounts_of(0)
    inject(3, 0, 4)
    for q in order:
        load(0, q).wait()
    for kind in (1, 2):
        for q in order:
            load(kind, q).wait()
    lateral(4, 0, 4)
    advance(3, 0)
    advance(3, 2)
    advance(3, 1)
    inject(2, 0, 4)

    @pl.when(has_far)
    def _():
        pl.semaphore_wait(barrier, 4)

    @pl.when(jnp.logical_not(has_far))
    def _():
        pl.semaphore_wait(barrier, 3)

    for c in range(CHUNKS):
        far_start(4, c)
    near_copy(4).start()
    inject(1, 0, 4)
    for c in range(CHUNKS):
        take(3, c)

    lateral(3, 0, 3)
    advance(2, 0)
    advance(2, 1)
    edge(3)
    take(2, 0)
    lateral(3, 3, 4)
    advance(2, 2)
    take(2, 1)
    edge(2)
    take(2, 2)
    take(2, 3)

    lateral(2, 0, 4)
    advance(1, 0)
    take(1, 0)
    advance(1, 1)
    take(1, 1)
    advance(1, 2)
    edge(1)
    inject(0, 0, 4)
    take(1, 2)
    take(1, 3)

    lateral(1, 2, 4)
    edge(0)
    tapers()
    for q in order:
        load(3, q).wait()
    imaging(3)
    reduce_start(3, 1)
    reduce_start(3, 0)
    lateral(1, 0, 2)
    advance(0, 2)
    imaging(2)
    reduce_start(2, 1)
    reduce_start(2, 0)
    advance(0, 0)
    take(0, 0)
    advance(0, 1)
    imaging(1)
    reduce_start(1, 1)
    take(0, 1)
    for block in range(BLOCKS):
        store(1, block)
    for block in range(1, BLOCKS):
        store(0, block)
    take(0, 2)
    take(0, 3)
    imaging(0)
    reduce_start(0, 1)
    reduce_start(1, 0)
    reduce_start(0, 0)
    store(0, 0)
    reduce_next(3)
    reduce_next(2)
    reduce_next(1)
    for level in (1, 2, 3, 4):
        near_copy(level).wait_send()

        @pl.when(has_far)
        def _():
            for c in range(CHUNKS):
                far_copy(level, c).wait_send()

    reduce_next(0)
    reduce_end(3)
    reduce_end(2)
    reduce_end(1)
    for block in range(BLOCKS):
        for side in range(2):
            first_copy(block, side, 0).wait_send()
            first_copy(block, side, 1).wait_send()
            second_copy(block, side).wait_send()
    reduce_end(0)


def write_out(gradient_ref, final_ref, gradient_hbm, final_hbm, sem):
    copies = [pltpu.make_async_copy(gradient_ref, gradient_hbm, sem.at[0])]
    half = final_ref.shape[1] // 2
    for level in range(2):
        for part in range(2):
            at = pl.ds(part * half, half)
            copies.append(
                pltpu.make_async_copy(
                    final_ref.at[level, at], final_hbm.at[0, level, at], sem.at[1 + 2 * level + part]
                )
            )
    for copy in copies:
        copy.start()
    for copy in copies:
        copy.wait()


def per_device(dom_size, courant_sq, adjoint_init, forward_saved, residual_traces, receivers, sources):
    planes, size_x, size_y = courant_sq.shape
    count = receivers.shape[1]
    f32, bf16 = jnp.float32, jnp.bfloat16
    padded = pltpu.VMEM((planes, size_x + 2 * PAD, size_y), f32)
    grid3 = (planes, size_x, size_y)
    dma = pltpu.SemaphoreType.DMA
    piece = (2, size_x // 4, size_y)
    gradient, final = pl.pallas_call(
        functools.partial(kernel, planes, size_x, size_y, dom_size),
        out_shape=(
            jax.ShapeDtypeStruct((planes, size_x // 4, size_y), f32),
            jax.ShapeDtypeStruct((2, planes, size_x, size_y), f32),
        ),
        in_specs=[pl.BlockSpec(memory_space=pltpu.HBM)] * 6,
        out_specs=(pl.BlockSpec(memory_space=pltpu.VMEM), pl.BlockSpec(memory_space=pltpu.VMEM)),
        scratch_shapes=[
            pltpu.VMEM((ITERS, count), f32),
            pltpu.VMEM((3, 1, count), jnp.int32),
            pltpu.SMEM((1, 3), jnp.int32),
        ]
        + [padded] * 5
        + [
            pltpu.VMEM(grid3, f32),
            pltpu.VMEM(grid3, f32),
            pltpu.VMEM((ITERS + 2,) + grid3, bf16),
            pltpu.VMEM(grid3, f32),
            pltpu.VMEM((2 * size_y, size_y), bf16),
            pltpu.VMEM((planes * size_x, count), bf16),
            pltpu.VMEM((size_x, count), bf16),
            pltpu.VMEM((ITERS, 2 * size_y, count), bf16),
            pltpu.VMEM(grid3, f32),
            pltpu.VMEM((planes, size_y), f32),
            pltpu.VMEM((size_x, size_y), f32),
            pltpu.VMEM((ITERS, WIDTH, size_x, size_y), f32),
            pltpu.VMEM((ITERS, WIDTH, size_x, size_y), f32),
            pltpu.VMEM((BLOCKS, 2, 2) + piece, f32),
            pltpu.VMEM((BLOCKS, 2) + piece, f32),
            pltpu.VMEM((BLOCKS, 2) + piece, f32),
            dma((4, planes)),
            dma((3,)),
            dma((ITERS, CHUNKS)),
            dma((ITERS, CHUNKS)),
            dma((ITERS,)),
            dma((ITERS,)),
            dma((BLOCKS, 2, 2)),
            dma((BLOCKS, 2, 2)),
            dma((BLOCKS, 2)),
            dma((BLOCKS, 2)),
        ],
        compiler_params=pltpu.CompilerParams(
            collective_id=0, has_side_effects=True, vmem_limit_bytes=34 * 1024 * 1024
        ),
    )(
        *(
            in_hbm(array)
            for array in (
                courant_sq,
                adjoint_init,
                forward_saved,
                residual_traces[0],
                receivers.transpose(2, 0, 1),
                sources,
            )
        )
    )
    return pl.pallas_call(
        write_out,
        out_shape=(
            jax.ShapeDtypeStruct(gradient.shape, f32),
            jax.ShapeDtypeStruct((1,) + final.shape, f32),
        ),
        in_specs=[pl.BlockSpec(memory_space=pltpu.VMEM)] * 2,
        out_specs=(pl.BlockSpec(memory_space=pl.ANY),) * 2,
        scratch_shapes=[dma((5,))],
        compiler_params=pltpu.CompilerParams(vmem_limit_bytes=8 * 1024 * 1024),
    )(gradient, final)


def solution(mesh):
    placed = (
        P(("groups", "dom"), None, None),
        P(("groups", "shot"), None, "dom", None, None),
        P(("groups", "shot"), None, "dom", None, None),
        P(("groups", "shot"), None, None),
        P(("groups", "shot"), None, None),
        P(("groups", "shot"), None),
    )
    return jax.shard_map(
        functools.partial(per_device, mesh.shape["dom"]),
        mesh=mesh,
        in_specs=placed,
        out_specs=(
            P(("groups", "dom"), "shot", None),
            P(("groups", "shot"), None, "dom", None, None),
        ),
        check_vma=False,
    )
```
